128 devices in a mesh: lat: 8 (over z, y_hi), lon: 16 (over x, y_lo, core).
Axes of the slice: x: 4, y: 4 (y_hi: 2, y_lo: 2; y = y_hi * 2 + y_lo), z: 4, core: 2. Of those that a mesh axis runs over, the one named last changes fastest.
Arguments:
- grid_feats: float32 [8, 32, 128, 1024], P('lat', 'lon'), may hold values from -6 to 6
- lift_index: int32 [8, 48, 4], P('lat', 'lon'), may hold values from 0 to 255, as said below
- lift_weight: float32 [8, 48, 4, 128, 128], P('lat', 'lon'), may hold values from -0.25 to 0.25
- window_index: int32 [8, 48, 8], P('lat', 'lon'), may hold values from 0 to 383, as said below
- window_count: int32 [8, 48], P('lat', 'lon'), may hold values from 4 to 8
- norm_gains: float32 [2, 1024], replicated, may hold values from 0.5 to 1.5
- qkv_weight: bfloat16 [1024, 3072], replicated, may hold values from -6.5 to 6.5
- out_weight: bfloat16 [1024, 1024], replicated, may hold values from -0.1875 to 0.1875
- up_weight: bfloat16 [1024, 2048], replicated, may hold values from -0.1875 to 0.1875
- down_weight: bfloat16 [2048, 1024], replicated, may hold values from -0.125 to 0.125
- return_index: int32 [8, 32, 4], P('lat', 'lon'), may hold values from 0 to 383, as said below
- return_weight: float32 [8, 32, 4, 128, 128], P('lat', 'lon'), may hold values from -0.25 to 0.25
Outputs:
- grid_out: float32 [8, 32, 128, 1024], P('lat', 'lon')
The draws below stay inside these ranges and needn't reach their ends.
Inputs may be any that keep to these rules, and one draw needn't show every extreme that they name: `lift_index`: entries name grid blocks a' * 32 + b'; the 4 entries of a row differ; for mesh block (a, c), |a' - a| <= 1 and b' lies among the 4 columns from c // 3 * 2 - 1 to c // 3 * 2 + 2, counted modulo 32. `window_index`: entries name mesh blocks a' * 48 + c'; slot 0 is the query block itself, the 8 entries of a row differ; |a' - a| <= 1 and c' lies among the 5 columns from c // 3 * 3 - 1 to c // 3 * 3 + 3, counted modulo 48. `return_index`: entries name mesh blocks a' * 48 + c'; the 4 entries of a row differ; for grid block (a, b), |a' - a| <= 1 and c' lies among the 5 columns from b // 2 * 3 - 1 to b // 2 * 3 + 3, counted modulo 48.
All inputs are finite; a program needn't handle non-finite values.
Results may differ from the reference program's by a relative error of at most 0.0035.
Values may be sent and summed in bfloat16 or wider, within the bound.
No kernel may reach another device: no remote copies, remote signals or barrier semaphores. Data moves between devices by JAX's collectives and lax.ppermute only.
A program may use at most 128 MiB of HBM per device.

```python
import jax
import jax.numpy as jnp
from jax import lax

HEADS = 16
C = 1024
FF = 2048
BLK = 128
K = 4
NW = 8
GLON = 2
MLON = 3
BANDS = 8
GRID_LON = 32
MESH_LON = 48


def pick_blocks(seed_key, target_lon, target_blocks, source_lon, source_blocks, pick_count, skip_self):
    across = source_blocks + 2
    band_index = jnp.arange(BANDS, dtype=jnp.int32).reshape(BANDS, 1, 1, 1)
    column_index = jnp.arange(target_lon, dtype=jnp.int32).reshape(1, target_lon, 1, 1)
    sector_index = column_index // target_blocks
    lat_step = jnp.arange(3, dtype=jnp.int32).reshape(1, 1, 3, 1)
    lon_step = jnp.arange(across, dtype=jnp.int32).reshape(1, 1, 1, across)
    source_band = band_index + lat_step - 1
    source_column = (sector_index * source_blocks + lon_step - 1) % source_lon
    usable = jnp.logical_and(source_band >= 0, source_band < BANDS)
    if skip_self:
        itself = jnp.logical_and(source_band == band_index, source_column == column_index)
        usable = jnp.logical_and(usable, jnp.logical_not(itself))
    full_shape = (BANDS, target_lon, 3, across)
    identity = jnp.broadcast_to(source_band * source_lon + source_column, full_shape)
    ordinal = jnp.broadcast_to(lat_step * across + lon_step, full_shape)
    jitter = jax.random.randint(seed_key, full_shape, 0, 1048576, dtype=jnp.int32)
    scores = jnp.where(usable, jitter * 64 + ordinal, -1)
    scores = scores.reshape(BANDS, target_lon, 3 * across)
    identity = identity.reshape(BANDS, target_lon, 3 * across)
    chosen_values, chosen_places = lax.top_k(scores, pick_count)
    return jnp.take_along_axis(identity, chosen_places, axis=-1).astype(jnp.int32)


def draw_lift_index(key, part):
    return pick_blocks(jax.random.fold_in(key, 11), MESH_LON, MLON, GRID_LON, GLON, K, False)


def draw_return_index(key, part):
    return pick_blocks(jax.random.fold_in(key, 12), GRID_LON, GLON, MESH_LON, MLON, K, False)


def draw_window_index(key, part):
    others = pick_blocks(jax.random.fold_in(key, 13), MESH_LON, MLON, MESH_LON, MLON, NW - 1, True)
    band_index = jnp.arange(BANDS, dtype=jnp.int32).reshape(BANDS, 1, 1)
    column_index = jnp.arange(MESH_LON, dtype=jnp.int32).reshape(1, MESH_LON, 1)
    itself = band_index * MESH_LON + column_index
    return jnp.concatenate([itself, others], axis=-1).astype(jnp.int32)


def draw_qkv_weight(key, part):
    standard = jnp.clip(jax.random.normal(jax.random.fold_in(key, 20), (C, 3 * C), dtype=jnp.float32), -6.0, 6.0) / jnp.sqrt(float(C))
    query_part = standard[:, :C] * 1.4
    value_part = standard[:, 2 * C:]
    key_part = standard[:, C:2 * C] * 1.4
    return jnp.concatenate([query_part, key_part, value_part], axis=1).astype(jnp.bfloat16)


def place_ends(array, stream_key, least, top_value):
    longest = array.shape.index(max(array.shape))
    spots = []
    for shift in (0, 1):
        where = [jax.random.randint(jax.random.fold_in(stream_key, axis), (), 0, length) for axis, length in enumerate(array.shape)]
        where[longest] = (where[longest] + shift) % array.shape[longest]
        spots.append(tuple(where))
    return array.at[spots[0]].set(least).at[spots[1]].set(top_value)


def block_scale(key, shape, shards, least, high):
    factor_of, own = 1.0, jax.random.fold_in(key, 6)
    for dim, blocks in shards:
        heights = jnp.exp(jax.random.uniform(jax.random.fold_in(own, dim), (blocks,), jnp.float32, least / len(shards), high / len(shards)))
        factor_of = factor_of * jnp.repeat(heights, shape[dim] // blocks).reshape([-1 if axis == dim else 1 for axis in range(len(shape))])
    return factor_of


def normal_values(rng, shape, scale, most, shards=(), held_as=jnp.bfloat16):
    result = jax.random.normal(rng, shape, jnp.float32) * scale
    if len(shards) > 0:
        result = block_scale(rng, shape, shards, -0.22, 0.18) * result
    return jnp.clip(result, min=-most, max=most).astype(held_as)


def setup_inputs(seed: int = 0) -> dict:
    arg_keys = jax.random.split(jax.random.key(seed), 13)
    return {
        "grid_feats": normal_values(arg_keys[0], (BANDS, GRID_LON, BLK, C), 1.0, 6.0, ((0, 8), (1, 16)), jnp.float32),
        "lift_index": draw_lift_index(jax.random.fold_in(arg_keys[12], 71), 0),
        "lift_weight": normal_values(arg_keys[2], (BANDS, MESH_LON, K, BLK, BLK), (K * BLK) ** -0.5, 0.25, ((0, 8), (1, 16)), jnp.float32),
        "window_index": draw_window_index(jax.random.fold_in(arg_keys[12], 71), 0),
        "window_count": place_ends(jax.random.randint(arg_keys[4], (BANDS, MESH_LON), NW // 2, NW + 1), jax.random.fold_in(arg_keys[4], 1), NW // 2, NW).astype(jnp.int32),
        "norm_gains": jnp.clip(1.0 + 0.1 * jax.random.normal(arg_keys[5], (2, C), jnp.float32), 0.5, 1.5),
        "qkv_weight": draw_qkv_weight(jax.random.fold_in(arg_keys[12], 71), 0),
        "out_weight": normal_values(arg_keys[7], (C, C), C ** -0.5, 0.1875),
        "up_weight": normal_values(arg_keys[8], (C, FF), C ** -0.5, 0.1875),
        "down_weight": normal_values(arg_keys[9], (FF, C), FF ** -0.5, 0.125),
        "return_index": draw_return_index(jax.random.fold_in(arg_keys[12], 71), 0),
        "return_weight": normal_values(arg_keys[11], (BANDS, GRID_LON, K, BLK, BLK), (K * BLK) ** -0.5, 0.25, ((0, 8), (1, 16)), jnp.float32),
    }


EPSILON = 1e-05

def layer_norm(values, gain):
    centred = values - lax.optimization_barrier(jnp.mean(values, axis=-1, keepdims=True))
    spread = lax.optimization_barrier(jnp.mean(centred * centred, axis=-1, keepdims=True))
    return (centred * lax.rsqrt(spread + EPSILON) * gain).astype(jnp.bfloat16)

def gelu_exact(values):
    return 0.5 * values * (1.0 + lax.erf(values * 0.7071067811865476))

def reference(grid_feats, lift_index, lift_weight, window_index, window_count, norm_gains, qkv_weight, out_weight, up_weight, down_weight, return_index, return_weight):
    feature_width = grid_feats.shape[-1]
    head_size = feature_width // HEADS
    grid_table = grid_feats.reshape(-1, BLK, feature_width)

    def lift_block(pair):
        slots, weight = pair
        return jnp.einsum('krs,ksc->rc', weight, grid_table[slots], precision=lax.Precision.HIGHEST)
    mesh_in = lax.map(lift_block, (lift_index.reshape(-1, K), lift_weight.reshape(-1, K, BLK, BLK)))
    normed = layer_norm(mesh_in, norm_gains[0]).reshape(-1, feature_width)
    projected = jnp.dot(normed, qkv_weight, preferred_element_type=jnp.float32).astype(jnp.bfloat16)
    projected = projected.reshape(-1, BLK, 3 * feature_width)

    def attend_block(triple):
        query_rows, slots, live_count = triple
        gathered = projected[slots]
        keys = gathered[:, :, feature_width:2 * feature_width].reshape(NW * BLK, HEADS, head_size).astype(jnp.float32)
        values = gathered[:, :, 2 * feature_width:].reshape(NW * BLK, HEADS, head_size).astype(jnp.float32)
        queries = query_rows[:, :feature_width].reshape(BLK, HEADS, head_size).astype(jnp.float32)
        scores = jnp.einsum('qhd,khd->hqk', queries, keys) * head_size ** (-0.5)
        live = jnp.arange(NW * BLK, dtype=jnp.int32) // BLK < live_count
        masked = jnp.where(live[None, None, :], scores, -1e+30)
        highest = lax.optimization_barrier(jnp.max(masked, axis=-1, keepdims=True))
        raw_weights = jnp.exp(masked - highest)
        weights = (raw_weights / lax.optimization_barrier(jnp.sum(raw_weights, axis=-1, keepdims=True))).astype(jnp.bfloat16)
        mixed_rows = jnp.einsum('hqk,khd->qhd', weights.astype(jnp.float32), values)
        return mixed_rows.astype(jnp.bfloat16).reshape(BLK, feature_width)
    mixed = lax.map(attend_block, (projected, window_index.reshape(-1, NW), window_count.reshape(-1)))
    mixed = mixed.reshape(-1, feature_width)
    after_attention = mesh_in.reshape(-1, feature_width) + jnp.dot(mixed, out_weight, preferred_element_type=jnp.float32)
    normed_again = layer_norm(after_attention, norm_gains[1])
    hidden_units = gelu_exact(jnp.dot(normed_again, up_weight, preferred_element_type=jnp.float32)).astype(jnp.bfloat16)
    mesh_out = after_attention + jnp.dot(hidden_units, down_weight, preferred_element_type=jnp.float32)
    mesh_table = mesh_out.reshape(-1, BLK, feature_width)

    def return_block(pair):
        slots, weight = pair
        return jnp.einsum('krs,ksc->rc', weight, mesh_table[slots], precision=lax.Precision.HIGHEST)
    grid_out = lax.map(return_block, (return_index.reshape(-1, K), return_weight.reshape(-1, K, BLK, BLK)))
    return grid_out.reshape(BANDS, GRID_LON, BLK, feature_width)
```

```python
import jax
import jax.numpy as jnp
from jax import lax
from jax.experimental import pallas as pl
from jax.experimental.pallas import tpu as pltpu
from jax.sharding import PartitionSpec as P

HEADS = 16
EPSILON = 1e-05
AXES = ("lat", "lon")


def far_band(band):
    return band - 1 if band % 2 == 0 else band + 1


def relay_band(band):
    return band + 2 if band % 2 == 0 else band - 2


def outer_sector(sector):
    return sector - 1 if sector % 2 == 0 else sector + 1


def move(values, band_of, sector_of):
    bands, sectors = lax.axis_size("lat"), lax.axis_size("lon")
    pairs = []
    for band in range(bands):
        for sector in range(sectors):
            target = band_of(band)
            if 0 <= target < bands:
                pairs.append((band * sectors + sector, target * sectors + sector_of(sector) % sectors))
    return lax.ppermute(values, AXES, pairs)


def same(index):
    return index


def pair(index):
    return index ^ 1


def exchange(blocks, even_sector):
    first, last = blocks[0], blocks[-1]
    edge_out = jnp.where(even_sector, first, last)
    near = [move(block, pair, same) for block in blocks]
    outer_own = move(edge_out, same, outer_sector)
    outer_near = move(edge_out, pair, outer_sector)
    outer_far = move(edge_out, far_band, outer_sector)
    far = [move(block, relay_band, same) for block in near]
    inner = [
        move(jnp.where(even_sector, group[-1], group[0]), same, pair) for group in (blocks, near, far)
    ]
    return near + far + [outer_own, outer_near, outer_far] + inner


def table_slots(global_ids, total_lon, blocks_here):
    band_here = lax.axis_index("lat")
    sector_here = lax.axis_index("lon")
    band_step = global_ids // total_lon - band_here
    column = (global_ids % total_lon - sector_here * blocks_here + 1) % total_lon
    near_step = jnp.where(band_here % 2 == 0, 1, -1)
    group = jnp.where(band_step == 0, 0, jnp.where(band_step == near_step, 1, 2))
    outer_column = jnp.where(sector_here % 2 == 0, 0, blocks_here + 1)
    inside = group * blocks_here + column - 1
    outside = 3 * blocks_here + jnp.where(column == outer_column, 0, 3) + group
    own_column = jnp.logical_and(column >= 1, column <= blocks_here)
    return jnp.where(own_column, inside, outside)


def fill_table(pieces, table, sems):
    copies = []
    start = 0
    for place, piece in enumerate(pieces):
        count = piece.shape[0]
        copies.append(pltpu.make_async_copy(piece, table.at[pl.ds(start, count)], sems.at[place]))
        start += count
    return copies


def normalise(values, gain):
    centred = values - jnp.mean(values, axis=-1, keepdims=True)
    spread = jnp.mean(centred * centred, axis=-1, keepdims=True)
    return (centred * lax.rsqrt(spread + EPSILON) * gain).astype(jnp.bfloat16)


def mix_blocks(slots, place, weight, table, gathered, split):
    count, rows, width = weight.shape
    for k in range(count):
        gathered[k * width:(k + 1) * width, :] = table[slots[place * count + k]]
        full = weight[k]
        upper = full.astype(jnp.bfloat16)
        split[0:rows, k * width:(k + 1) * width] = upper
        split[rows:2 * rows, k * width:(k + 1) * width] = (full - upper.astype(jnp.float32)).astype(jnp.bfloat16)
    both = jnp.dot(split[...], gathered[...], preferred_element_type=jnp.float32)
    return both[:rows] + both[rows:]


def lift_kernel(slots, *refs, piece_count):
    pieces = refs[:piece_count]
    weight, gains, mesh_in, normed, table, gathered, split, sems = refs[piece_count:]
    copies = fill_table(pieces, table, sems)
    for copy in copies:
        copy.start()
    for copy in copies:
        copy.wait()
    for m in range(weight.shape[0]):
        mixed = mix_blocks(slots, m, weight[m], table, gathered, split)
        mesh_in[m] = mixed
        normed[m] = normalise(mixed, gains[0:1, :])


def return_kernel(slots, *refs, piece_count):
    pieces = refs[:piece_count]
    weight, out, table, gathered, split, sems = refs[piece_count:]
    copies = fill_table(pieces, table, sems)
    for copy in copies:
        copy.start()
    for copy in copies:
        copy.wait()
    for g in range(weight.shape[0]):
        out[g] = mix_blocks(slots, g, weight[g], table, gathered, split)


def layer_kernel(slots, counts, *refs, piece_count):
    pieces = refs[:piece_count]
    (
        queries, mesh_in, gains, out_hbm, up_hbm, down_hbm, mesh_out,
        table, gathered, mixed, out_weight, up_weight, down_weight, sems,
    ) = refs[piece_count:]
    copies = fill_table(pieces, table, sems)
    weights = [
        pltpu.make_async_copy(out_hbm, out_weight, sems.at[piece_count]),
        pltpu.make_async_copy(up_hbm, up_weight, sems.at[piece_count + 1]),
        pltpu.make_async_copy(down_hbm, down_weight, sems.at[piece_count + 2]),
    ]
    for copy in copies + weights:
        copy.start()
    for copy in copies:
        copy.wait()
    mesh_blocks, rows, width = mesh_in.shape
    neighbours = gathered.shape[0] // rows
    head_size = width // HEADS
    scale = head_size ** (-0.5)
    lane = lax.broadcasted_iota(jnp.int32, (rows, 2 * head_size), 1)
    low_half = lane < head_size
    key_block = lax.broadcasted_iota(jnp.int32, (1, neighbours * rows), 1) // rows

    def attend(m, carry):
        for j in range(neighbours):
            gathered[j * rows:(j + 1) * rows, :] = table[slots[m * neighbours + j]]
        bias = jnp.where(key_block < counts[m], 0.0, -1e30)
        for h in range(HEADS // 2):
            at = h * 2 * head_size
            query = queries[m, :, at:at + 2 * head_size]
            keys = gathered[:, at:at + 2 * head_size]
            values = gathered[:, width + at:width + at + 2 * head_size]
            parts = []
            for half in range(2):
                chosen = low_half if half == 0 else jnp.logical_not(low_half)
                one = jnp.where(chosen, query, jnp.zeros_like(query))
                scores = lax.dot_general(
                    one, keys, (((1,), (1,)), ((), ())), preferred_element_type=jnp.float32
                )
                scores = scores * scale + bias
                highest = jnp.max(scores, axis=-1, keepdims=True)
                raw = jnp.exp(scores - highest)
                total = jnp.sum(raw, axis=-1, keepdims=True)
                part = jnp.dot(raw.astype(jnp.bfloat16), values, preferred_element_type=jnp.float32)
                parts.append(part / total)
            mixed[pl.ds(m * rows, rows), at:at + 2 * head_size] = jnp.where(
                low_half, parts[0], parts[1]
            ).astype(jnp.bfloat16)
        return carry

    lax.fori_loop(0, mesh_blocks, attend, 0)
    for copy in weights:
        copy.wait()
    after = mesh_in[...].reshape(mesh_blocks * rows, width) + jnp.dot(
        mixed[...], out_weight[...], preferred_element_type=jnp.float32
    )
    again = normalise(after, gains[1:2, :])
    hidden = jnp.dot(again, up_weight[...], preferred_element_type=jnp.float32)
    hidden = (0.5 * hidden * (1.0 + lax.erf(hidden * 0.7071067811865476))).astype(jnp.bfloat16)
    result = after + jnp.dot(hidden, down_weight[...], preferred_element_type=jnp.float32)
    mesh_out[...] = result.astype(jnp.bfloat16).reshape(mesh_blocks, rows, width)


def any_specs(count):
    return [pl.BlockSpec(memory_space=pl.ANY)] * count


VMEM_SPEC = pl.BlockSpec(memory_space=pltpu.MemorySpace.VMEM)


def shards(
    grid_feats, lift_index, lift_weight, window_index, window_count, norm_gains,
    qkv_weight, out_weight, up_weight, down_weight, return_index, return_weight,
):
    even_sector = lax.axis_index("lon") % 2 == 0
    lon_count = lax.axis_size("lon")
    grid_blocks = grid_feats.shape[1]
    mesh_blocks = lift_index.shape[1]
    rows, width = grid_feats.shape[2:]
    grid_lon = grid_blocks * lon_count
    mesh_lon = mesh_blocks * lon_count
    bf16, f32 = jnp.bfloat16, jnp.float32
    mesh_table = 3 * mesh_blocks + 6
    grid_table = 3 * grid_blocks + 6

    grid_bf16 = grid_feats[0].astype(bf16)
    grid_parts = [grid_bf16[i:i + 1] for i in range(grid_blocks)]
    grid_pieces = [grid_bf16] + exchange(grid_parts, even_sector)
    lift_slots = table_slots(lift_index[0], grid_lon, grid_blocks).reshape(-1)
    picks = lift_weight.shape[2]
    mesh_in, normed = pl.pallas_call(
        lambda *refs: lift_kernel(*refs, piece_count=len(grid_pieces)),
        grid_spec=pltpu.PrefetchScalarGridSpec(
            num_scalar_prefetch=1,
            in_specs=any_specs(len(grid_pieces)) + [VMEM_SPEC, VMEM_SPEC],
            out_specs=[VMEM_SPEC, VMEM_SPEC],
            scratch_shapes=[
                pltpu.VMEM((grid_table, rows, width), bf16),
                pltpu.VMEM((picks * rows, width), bf16),
                pltpu.VMEM((2 * rows, picks * rows), bf16),
                pltpu.SemaphoreType.DMA((len(grid_pieces),)),
            ],
        ),
        out_shape=[
            jax.ShapeDtypeStruct((mesh_blocks, rows, width), f32),
            jax.ShapeDtypeStruct((mesh_blocks, rows, width), bf16),
        ],
        name="lift",
    )(lift_slots, *grid_pieces, lift_weight[0], norm_gains)

    normed_parts = [normed[i:i + 1] for i in range(mesh_blocks)]
    halo = exchange(normed_parts, even_sector)
    own = jnp.dot(
        normed.reshape(-1, width), qkv_weight, preferred_element_type=f32
    ).astype(bf16)
    queries = own[:, :width].reshape(mesh_blocks, rows, width)
    kv_weight = qkv_weight[:, width:]
    kv_pieces = [own[:, width:].reshape(mesh_blocks, rows, 2 * width)]
    groups = [halo[:mesh_blocks], halo[mesh_blocks:2 * mesh_blocks], halo[2 * mesh_blocks:]]
    for group in groups:
        stacked = jnp.concatenate(group, axis=0)
        kv_pieces.append(
            jnp.dot(stacked.reshape(-1, width), kv_weight, preferred_element_type=f32)
            .astype(bf16)
            .reshape(-1, rows, 2 * width)
        )
    window_slots = table_slots(window_index[0], mesh_lon, mesh_blocks).reshape(-1)
    neighbours = window_index.shape[2]
    hidden_width = up_weight.shape[1]
    mesh_out = pl.pallas_call(
        lambda *refs: layer_kernel(*refs, piece_count=len(kv_pieces)),
        grid_spec=pltpu.PrefetchScalarGridSpec(
            num_scalar_prefetch=2,
            in_specs=any_specs(len(kv_pieces)) + [VMEM_SPEC] * 3 + any_specs(3),
            out_specs=VMEM_SPEC,
            scratch_shapes=[
                pltpu.VMEM((mesh_table, rows, 2 * width), bf16),
                pltpu.VMEM((neighbours * rows, 2 * width), bf16),
                pltpu.VMEM((mesh_blocks * rows, width), bf16),
                pltpu.VMEM((width, width), bf16),
                pltpu.VMEM((width, hidden_width), bf16),
                pltpu.VMEM((hidden_width, width), bf16),
                pltpu.SemaphoreType.DMA((len(kv_pieces) + 3,)),
            ],
        ),
        out_shape=jax.ShapeDtypeStruct((mesh_blocks, rows, width), bf16),
        name="layer",
    )(
        window_slots, window_count[0], *kv_pieces, queries, mesh_in, norm_gains,
        out_weight, up_weight, down_weight,
    )

    mesh_parts = [mesh_out[i:i + 1] for i in range(mesh_blocks)]
    mesh_pieces = [mesh_out] + exchange(mesh_parts, even_sector)
    return_slots = table_slots(return_index[0], mesh_lon, mesh_blocks).reshape(-1)
    grid_out = pl.pallas_call(
        lambda *refs: return_kernel(*refs, piece_count=len(mesh_pieces)),
        grid_spec=pltpu.PrefetchScalarGridSpec(
            num_scalar_prefetch=1,
            in_specs=any_specs(len(mesh_pieces)) + [VMEM_SPEC],
            out_specs=VMEM_SPEC,
            scratch_shapes=[
                pltpu.VMEM((mesh_table, rows, width), bf16),
                pltpu.VMEM((picks * rows, width), bf16),
                pltpu.VMEM((2 * rows, picks * rows), bf16),
                pltpu.SemaphoreType.DMA((len(mesh_pieces),)),
            ],
        ),
        out_shape=jax.ShapeDtypeStruct((grid_blocks, rows, width), f32),
        name="give_back",
    )(return_slots, *mesh_pieces, return_weight[0])
    return grid_out.reshape(1, grid_blocks, rows, width)


def solution(mesh):
    placed = (
        P("lat", "lon", None, None),
        P("lat", "lon", None),
        P("lat", "lon", None, None, None),
        P("lat", "lon", None),
        P("lat", "lon"),
        P(),
        P(),
        P(),
        P(),
        P(),
        P("lat", "lon", None),
        P("lat", "lon", None, None, None),
    )
    return jax.shard_map(
        shards, mesh=mesh, in_specs=placed, out_specs=P("lat", "lon", None, None), check_vma=False
    )
```

```python
import jax
import jax.numpy as jnp
from jax import lax
from jax.experimental import pallas as pl
from jax.experimental.pallas import tpu as pltpu
from jax.sharding import PartitionSpec as P


HEADS = 16
EPSILON = 1e-05
AXES = ("lat", "lon")
GRID_SCALE = 8192.0


def far_band(band):
    return band - 1 if band % 2 == 0 else band + 1


def relay_band(band):
    return band + 2 if band % 2 == 0 else band - 2


def outer_sector(sector):
    return sector - 1 if sector % 2 == 0 else sector + 1


def move(values, band_of, sector_of):
    bands, sectors = lax.axis_size("lat"), lax.axis_size("lon")
    pairs = []
    for band in range(bands):
        for sector in range(sectors):
            target = band_of(band)
            if 0 <= target < bands:
                pairs.append((band * sectors + sector, target * sectors + sector_of(sector) % sectors))
    return lax.ppermute(values, AXES, pairs)


def same(index):
    return index


def pair(index):
    return index ^ 1


def exchange(blocks, even_sector):
    last = blocks.shape[0] - 1
    parts = (blocks[:last], blocks[last:])

    def inner_edge(halves):
        return jnp.where(even_sector, halves[1], halves[0][:1])

    edge_out = jnp.where(even_sector, parts[0][:1], parts[1])
    near = [move(part, pair, same) for part in parts]
    outer = [
        move(edge_out, same, outer_sector), move(edge_out, pair, outer_sector), move(edge_out, far_band, outer_sector)
    ]
    far = [move(part, relay_band, same) for part in near]
    inner = [
        move(jnp.concatenate([inner_edge(parts), inner_edge(near)], axis=0), same, pair),
        move(inner_edge(far), same, pair),
    ]
    return near, far, outer, inner


def table_slots(global_ids, total_lon, blocks_here):
    band_here = lax.axis_index("lat")
    sector_here = lax.axis_index("lon")
    band_step = global_ids // total_lon - band_here
    column = (global_ids % total_lon - sector_here * blocks_here + 1) % total_lon
    near_step = jnp.where(band_here % 2 == 0, 1, -1)
    group = jnp.where(band_step == 0, 0, jnp.where(band_step == near_step, 1, 2))
    outer_column = jnp.where(sector_here % 2 == 0, 0, blocks_here + 1)
    inside = group * blocks_here + column - 1
    outside = 3 * blocks_here + jnp.where(column == outer_column, 0, 3) + group
    own_column = jnp.logical_and(column >= 1, column <= blocks_here)
    return jnp.where(own_column, inside, outside)


def fill_table(pieces, table, sems):
    copies = []
    start = 0
    for place, piece in enumerate(pieces):
        count = piece.shape[0]
        copies.append(pltpu.make_async_copy(piece, table.at[pl.ds(start, count)], sems.at[place]))
        start += count
    return copies


def normalise(values, gain):
    centred = values - jnp.mean(values, axis=-1, keepdims=True)
    spread = jnp.mean(centred * centred, axis=-1, keepdims=True)
    return (centred * lax.rsqrt(spread + EPSILON) * gain).astype(jnp.bfloat16)


def split_weights(weight, split):
    count, rows, width = weight.shape
    for k in range(count):
        full = weight[k]
        upper = full.astype(jnp.bfloat16)
        split[0:rows, k * width:(k + 1) * width] = upper
        split[rows:2 * rows, k * width:(k + 1) * width] = (full - upper.astype(jnp.float32)).astype(jnp.bfloat16)


def mix_blocks(slots, place, weight, table, upper, lower, split):
    count, rows, width = weight.shape
    split_weights(weight, split)
    for k in range(count):
        block = table[slots[place * count + k]]
        high = block.astype(jnp.bfloat16)
        upper[k * width:(k + 1) * width, :] = high
        if lower is not None:
            lower[k * width:(k + 1) * width, :] = (block - high.astype(jnp.float32)).astype(jnp.bfloat16)
    both = jnp.dot(split[...], upper[...], preferred_element_type=jnp.float32)
    total = both[:rows] + both[rows:]
    if lower is not None:
        total = total + jnp.dot(split[0:rows, :], lower[...], preferred_element_type=jnp.float32)
    return total


def lift_kernel(slots, *refs, piece_count):
    pieces = refs[:piece_count]
    weight, gains, mesh_in, normed, table, upper, lower, split, sems = refs[piece_count:]
    copies = fill_table(pieces, table, sems)
    for copy in copies:
        copy.start()
    for copy in copies:
        copy.wait()
    for m in range(weight.shape[0]):
        mixed = mix_blocks(slots, m, weight.at[m], table, upper, lower, split)
        mesh_in[m] = mixed
        normed[m] = normalise(mixed, gains[0:1, :])


def return_kernel(slots, *refs, piece_count):
    pieces = refs[:piece_count]
    weight, out, table, upper, split, sems = refs[piece_count:]
    copies = fill_table(pieces, table, sems)
    for copy in copies:
        copy.start()
    for copy in copies:
        copy.wait()
    for g in range(weight.shape[0]):
        out[g] = mix_blocks(slots, g, weight.at[g], table, upper, None, split)


def layer_kernel(slots, counts, *refs, piece_count):
    pieces = refs[:piece_count]
    (
        queries, mesh_in, gains, out_hbm, up_hbm, down_hbm, mesh_out,
        table, keys, values, mixed, out_weight, up_weight, down_weight, sems,
    ) = refs[piece_count:]
    copies = fill_table(pieces, table, sems)
    weights = [
        pltpu.make_async_copy(out_hbm, out_weight, sems.at[piece_count]),
        pltpu.make_async_copy(up_hbm, up_weight, sems.at[piece_count + 1]),
        pltpu.make_async_copy(down_hbm, down_weight, sems.at[piece_count + 2]),
    ]
    for copy in copies + weights:
        copy.start()
    for copy in copies:
        copy.wait()
    mesh_blocks, rows, width = mesh_in.shape
    neighbours = keys.shape[0] // rows
    head_size = width // HEADS
    wide = 2 * head_size
    certain = neighbours // 2 * rows
    low_half = lax.broadcasted_iota(jnp.int32, (rows, wide), 1) < head_size
    key_block = lax.broadcasted_iota(jnp.int32, (1, neighbours * rows - certain), 1) // rows + neighbours // 2
    values[:, :, wide:] = jnp.ones((HEADS // 2, neighbours * rows, wide), jnp.bfloat16)

    def attend(m, carry):
        for j in range(neighbours):
            slot = slots[m * neighbours + j]
            keys[j * rows:(j + 1) * rows, :] = table[slot, :, 0:width]
            for h in range(HEADS // 2):
                at = width + h * wide
                values[h, j * rows:(j + 1) * rows, 0:wide] = table[slot, :, at:at + wide]
        bias = jnp.where(key_block < counts[m], 0.0, -1e30)
        for h in range(HEADS // 2):
            at = h * wide
            query = queries[m, :, at:at + wide] * jnp.asarray(head_size ** (-0.5), jnp.bfloat16)
            none = jnp.zeros_like(query)
            pair_rows = jnp.concatenate(
                [jnp.where(low_half, query, none), jnp.where(low_half, none, query)], axis=0
            )
            scores = lax.dot_general(
                pair_rows, keys[:, at:at + wide], (((1,), (1,)), ((), ())), preferred_element_type=jnp.float32
            )
            first, second = scores[:, :certain], scores[:, certain:] + bias
            highest = jnp.maximum(
                jnp.max(first, axis=-1, keepdims=True), jnp.max(second, axis=-1, keepdims=True)
            )
            raw = jnp.concatenate(
                [jnp.exp(first - highest).astype(jnp.bfloat16), jnp.exp(second - highest).astype(jnp.bfloat16)],
                axis=1,
            )
            summed = jnp.dot(raw, values[h], preferred_element_type=jnp.float32)
            part = summed[:, :wide] / summed[:, wide:]
            mixed[pl.ds(m * rows, rows), at:at + wide] = jnp.where(
                low_half, part[:rows], part[rows:]
            ).astype(jnp.bfloat16)
        return carry

    lax.fori_loop(0, mesh_blocks, attend, 0)
    for copy in weights:
        copy.wait()
    after = mesh_in[...].reshape(mesh_blocks * rows, width) + jnp.dot(
        mixed[...], out_weight[...], preferred_element_type=jnp.float32
    )
    again = normalise(after, gains[1:2, :])
    hidden = jnp.dot(again, up_weight[...], preferred_element_type=jnp.float32)
    hidden = (0.5 * hidden * (1.0 + lax.erf(hidden * 0.7071067811865476))).astype(jnp.bfloat16)
    result = after + jnp.dot(hidden, down_weight[...], preferred_element_type=jnp.float32)
    mesh_out[...] = result.astype(jnp.bfloat16).reshape(mesh_blocks, rows, width)


def any_specs(count):
    return [pl.BlockSpec(memory_space=pl.ANY)] * count


VMEM_SPEC = pl.BlockSpec(memory_space=pltpu.MemorySpace.VMEM)


def shards(
    grid_feats, lift_index, lift_weight, window_index, window_count, norm_gains,
    qkv_weight, out_weight, up_weight, down_weight, return_index, return_weight,
):
    even_sector = lax.axis_index("lon") % 2 == 0
    lon_count = lax.axis_size("lon")
    grid_blocks = grid_feats.shape[1]
    mesh_blocks = lift_index.shape[1]
    rows, width = grid_feats.shape[2:]
    grid_lon = grid_blocks * lon_count
    mesh_lon = mesh_blocks * lon_count
    bf16, f32 = jnp.bfloat16, jnp.float32
    mesh_table = 3 * mesh_blocks + 6
    grid_table = 3 * grid_blocks + 6

    own_grid = grid_feats[0]
    sent = (own_grid * GRID_SCALE).astype(jnp.float16)
    near, far, outer, inner = exchange(sent, even_sector)
    grid_pieces = [own_grid] + [
        piece.astype(f32) * (1.0 / GRID_SCALE) for piece in near + far + outer + inner
    ]
    lift_slots = table_slots(lift_index[0], grid_lon, grid_blocks).reshape(-1)
    picks = lift_weight.shape[2]
    mesh_in, normed = pl.pallas_call(
        lambda *refs: lift_kernel(*refs, piece_count=len(grid_pieces)),
        grid_spec=pltpu.PrefetchScalarGridSpec(
            num_scalar_prefetch=1,
            in_specs=any_specs(len(grid_pieces)) + [VMEM_SPEC, VMEM_SPEC],
            out_specs=[VMEM_SPEC, VMEM_SPEC],
            scratch_shapes=[
                pltpu.VMEM((grid_table, rows, width), f32),
                pltpu.VMEM((picks * rows, width), bf16),
                pltpu.VMEM((picks * rows, width), bf16),
                pltpu.VMEM((2 * rows, picks * rows), bf16),
                pltpu.SemaphoreType.DMA((len(grid_pieces),)),
            ],
        ),
        out_shape=[
            jax.ShapeDtypeStruct((mesh_blocks, rows, width), f32),
            jax.ShapeDtypeStruct((mesh_blocks, rows, width), bf16),
        ],
        name="lift",
    )(lift_slots, *grid_pieces, lift_weight[0], norm_gains)

    near, far, outer, inner = exchange(normed, even_sector)
    own = jnp.dot(normed.reshape(-1, width), qkv_weight, preferred_element_type=f32).astype(bf16)
    queries = own[:, :width].reshape(mesh_blocks, rows, width)
    kv_weight = qkv_weight[:, width:]
    kv_pieces = [own[:, width:].reshape(mesh_blocks, rows, 2 * width)]

    def project(group):
        stacked = jnp.concatenate(group, axis=0) if len(group) > 1 else group[0]
        return (
            jnp.dot(stacked.reshape(-1, width), kv_weight, preferred_element_type=f32)
            .astype(bf16)
            .reshape(-1, rows, 2 * width)
        )

    kv_pieces.append(project(near))
    side = project(outer + inner[:1])
    kv_pieces.append(project(far))
    kv_pieces.append(side)
    kv_pieces.append(project(inner[1:]))
    window_slots = table_slots(window_index[0], mesh_lon, mesh_blocks).reshape(-1)
    neighbours = window_index.shape[2]
    hidden_width = up_weight.shape[1]
    mesh_out = pl.pallas_call(
        lambda *refs: layer_kernel(*refs, piece_count=len(kv_pieces)),
        grid_spec=pltpu.PrefetchScalarGridSpec(
            num_scalar_prefetch=2,
            in_specs=any_specs(len(kv_pieces)) + [VMEM_SPEC] * 3 + any_specs(3),
            out_specs=VMEM_SPEC,
            scratch_shapes=[
                pltpu.VMEM((mesh_table, rows, 2 * width), bf16),
                pltpu.VMEM((neighbours * rows, width), bf16),
                pltpu.VMEM((HEADS // 2, neighbours * rows, 4 * (width // HEADS)), bf16),
                pltpu.VMEM((mesh_blocks * rows, width), bf16),
                pltpu.VMEM((width, width), bf16),
                pltpu.VMEM((width, hidden_width), bf16),
                pltpu.VMEM((hidden_width, width), bf16),
                pltpu.SemaphoreType.DMA((len(kv_pieces) + 3,)),
            ],
        ),
        out_shape=jax.ShapeDtypeStruct((mesh_blocks, rows, width), bf16),
        name="layer",
    )(
        window_slots, window_count[0], *kv_pieces, queries, mesh_in, norm_gains,
        out_weight, up_weight, down_weight,
    )

    near, far, outer, inner = exchange(mesh_out, even_sector)
    mesh_pieces = [mesh_out] + near + far + outer + inner
    return_slots = table_slots(return_index[0], mesh_lon, mesh_blocks).reshape(-1)
    grid_out = pl.pallas_call(
        lambda *refs: return_kernel(*refs, piece_count=len(mesh_pieces)),
        grid_spec=pltpu.PrefetchScalarGridSpec(
            num_scalar_prefetch=1,
            in_specs=any_specs(len(mesh_pieces)) + [VMEM_SPEC],
            out_specs=VMEM_SPEC,
            scratch_shapes=[
                pltpu.VMEM((mesh_table, rows, width), bf16),
                pltpu.VMEM((picks * rows, width), bf16),
                pltpu.VMEM((2 * rows, picks * rows), bf16),
                pltpu.SemaphoreType.DMA((len(mesh_pieces),)),
            ],
        ),
        out_shape=jax.ShapeDtypeStruct((grid_blocks, rows, width), f32),
        name="give_back",
    )(return_slots, *mesh_pieces, return_weight[0])
    return grid_out.reshape(1, grid_blocks, rows, width)


def solution(mesh):
    placed = (
        P("lat", "lon", None, None),
        P("lat", "lon", None),
        P("lat", "lon", None, None, None),
        P("lat", "lon", None),
        P("lat", "lon"),
        P(),
        P(),
        P(),
        P(),
        P(),
        P("lat", "lon", None),
        P("lat", "lon", None, None, None),
    )

    return jax.shard_map(shards, mesh=mesh, in_specs=placed, out_specs=P("lat", "lon", None, None), check_vma=False)
```

```python
import jax
import jax.numpy as jnp
from jax import lax
from jax.experimental import pallas as pl
from jax.experimental.pallas import tpu as pltpu
from jax.sharding import PartitionSpec as P


HEADS = 16
EPSILON = 1e-05
AXES = ("lat", "lon")
GRID_SCALE = 8192.0


def far_band(band):
    return band - 1 if band % 2 == 0 else band + 1


def relay_band(band):
    return band + 2 if band % 2 == 0 else band - 2


def outer_sector(sector):
    return sector - 1 if sector % 2 == 0 else sector + 1


def move(values, band_of, sector_of):
    bands, sectors = lax.axis_size("lat"), lax.axis_size("lon")
    pairs = []
    for band in range(bands):
        for sector in range(sectors):
            target = band_of(band)
            if 0 <= target < bands:
                pairs.append((band * sectors + sector, target * sectors + sector_of(sector) % sectors))
    return lax.ppermute(values, AXES, pairs)


def same(index):
    return index


def pair(index):
    return index ^ 1


def exchange(parts, edge_out, even_sector):
    def inner_edge(halves):
        return jnp.where(even_sector, halves[1], halves[0][:1])

    near = [move(part, pair, same) for part in parts]
    outer = [
        move(edge_out, same, outer_sector), move(edge_out, pair, outer_sector), move(edge_out, far_band, outer_sector)
    ]
    far = [move(part, relay_band, same) for part in near]
    inner = [
        move(jnp.concatenate([inner_edge(parts), inner_edge(near)], axis=0), same, pair),
        move(inner_edge(far), same, pair),
    ]
    return near, far, outer, inner


def table_slots(global_ids, total_lon, blocks_here):
    band_here = lax.axis_index("lat")
    sector_here = lax.axis_index("lon")
    band_step = global_ids // total_lon - band_here
    column = (global_ids % total_lon - sector_here * blocks_here + 1) % total_lon
    near_step = jnp.where(band_here % 2 == 0, 1, -1)
    group = jnp.where(band_step == 0, 0, jnp.where(band_step == near_step, 1, 2))
    outer_column = jnp.where(sector_here % 2 == 0, 0, blocks_here + 1)
    inside = group * blocks_here + column - 1
    outside = 3 * blocks_here + jnp.where(column == outer_column, 0, 3) + group
    own_column = jnp.logical_and(column >= 1, column <= blocks_here)
    return jnp.where(own_column, inside, outside)


def fill_table(pieces, table, sems):
    copies = []
    start = 0
    for place, piece in enumerate(pieces):
        count = piece.shape[0]
        copies.append(pltpu.make_async_copy(piece, table.at[pl.ds(start, count)], sems.at[place]))
        start += count
    return copies


def normalise(values, gain):
    centred = values - jnp.mean(values, axis=-1, keepdims=True)
    spread = jnp.mean(centred * centred, axis=-1, keepdims=True)
    return (centred * lax.rsqrt(spread + EPSILON) * gain).astype(jnp.bfloat16)


def split_weights(weight, split):
    count, rows, width = weight.shape
    for k in range(count):
        full = weight[k]
        upper = full.astype(jnp.bfloat16)
        split[0:rows, k * width:(k + 1) * width] = upper
        split[rows:2 * rows, k * width:(k + 1) * width] = (full - upper.astype(jnp.float32)).astype(jnp.bfloat16)


def mix_blocks(slots, place, weight, table, upper, lower, split):
    count, rows, width = weight.shape
    split_weights(weight, split)
    for k in range(count):
        block = table[slots[place * count + k]]
        high = block.astype(jnp.bfloat16)
        upper[k * width:(k + 1) * width, :] = high
        if lower is not None:
            lower[k * width:(k + 1) * width, :] = (block - high.astype(jnp.float32)).astype(jnp.bfloat16)
    both = jnp.dot(split[...], upper[...], preferred_element_type=jnp.float32)
    total = both[:rows] + both[rows:]
    if lower is not None:
        total = total + jnp.dot(split[0:rows, :], lower[...], preferred_element_type=jnp.float32)
    return total


def store_part(place, count, even, value, head, tail, edge):
    if place < count - 1:
        head[place] = value
    else:
        tail[0] = value
    if place in (0, count - 1):
        @pl.when(even == (1 if place == 0 else 0))
        def _():
            edge[0] = value


def lift_kernel(slots, even, *refs, piece_count):
    pieces = refs[:piece_count]
    weight, gains, mesh_in, normed, head, tail, edge, table, upper, lower, split, sems = refs[piece_count:]
    copies = fill_table(pieces, table, sems)
    for copy in copies:
        copy.start()
    for copy in copies:
        copy.wait()
    for m in range(weight.shape[0]):
        mixed = mix_blocks(slots, m, weight.at[m], table, upper, lower, split)
        mesh_in[m] = mixed
        result = normalise(mixed, gains[0:1, :])
        normed[m] = result
        store_part(m, weight.shape[0], even[0], result, head, tail, edge)


def return_kernel(slots, *refs, piece_count):
    pieces = refs[:piece_count]
    weight, out, table, upper, split, sems = refs[piece_count:]
    copies = fill_table(pieces, table, sems)
    for copy in copies:
        copy.start()
    for copy in copies:
        copy.wait()
    for g in range(weight.shape[0]):
        out[g] = mix_blocks(slots, g, weight.at[g], table, upper, None, split)


def layer_kernel(slots, counts, even, *refs, piece_count):
    pieces = refs[:piece_count]
    (
        queries, mesh_in, gains, out_hbm, up_hbm, down_hbm, head, tail, edge,
        table, keys, values, mixed, out_weight, up_weight, down_weight, sems,
    ) = refs[piece_count:]
    copies = fill_table(pieces, table, sems)
    weights = [
        pltpu.make_async_copy(out_hbm, out_weight, sems.at[piece_count]),
        pltpu.make_async_copy(up_hbm, up_weight, sems.at[piece_count + 1]),
        pltpu.make_async_copy(down_hbm, down_weight, sems.at[piece_count + 2]),
    ]
    for copy in copies + weights:
        copy.start()
    for copy in copies:
        copy.wait()
    mesh_blocks, rows, width = mesh_in.shape
    neighbours = keys.shape[0] // rows
    head_size = width // HEADS
    wide = 2 * head_size
    certain = neighbours // 2 * rows
    low_half = lax.broadcasted_iota(jnp.int32, (rows, wide), 1) < head_size
    key_block = lax.broadcasted_iota(jnp.int32, (1, neighbours * rows - certain), 1) // rows + neighbours // 2
    values[:, :, wide:] = jnp.ones((HEADS // 2, neighbours * rows, wide), jnp.bfloat16)

    def attend(m, carry):
        for j in range(neighbours):
            slot = slots[m * neighbours + j]
            keys[j * rows:(j + 1) * rows, :] = table[slot, :, 0:width]
            for h in range(HEADS // 2):
                at = width + h * wide
                values[h, j * rows:(j + 1) * rows, 0:wide] = table[slot, :, at:at + wide]
        bias = jnp.where(key_block < counts[m], 0.0, -1e30)
        for h in range(HEADS // 2):
            at = h * wide
            query = queries[m, :, at:at + wide] * jnp.asarray(head_size ** (-0.5), jnp.bfloat16)
            none = jnp.zeros_like(query)
            pair_rows = jnp.concatenate(
                [jnp.where(low_half, query, none), jnp.where(low_half, none, query)], axis=0
            )
            scores = lax.dot_general(
                pair_rows, keys[:, at:at + wide], (((1,), (1,)), ((), ())), preferred_element_type=jnp.float32
            )
            first, second = scores[:, :certain], scores[:, certain:] + bias
            highest = jnp.maximum(
                jnp.max(first, axis=-1, keepdims=True), jnp.max(second, axis=-1, keepdims=True)
            )
            raw = jnp.concatenate(
                [jnp.exp(first - highest).astype(jnp.bfloat16), jnp.exp(second - highest).astype(jnp.bfloat16)],
                axis=1,
            )
            summed = jnp.dot(raw, values[h], preferred_element_type=jnp.float32)
            part = summed[:, :wide] / summed[:, wide:]
            mixed[pl.ds(m * rows, rows), at:at + wide] = jnp.where(
                low_half, part[:rows], part[rows:]
            ).astype(jnp.bfloat16)
        return carry

    lax.fori_loop(0, mesh_blocks, attend, 0)
    for copy in weights:
        copy.wait()
    after = mesh_in[...].reshape(mesh_blocks * rows, width) + jnp.dot(
        mixed[...], out_weight[...], preferred_element_type=jnp.float32
    )
    again = normalise(after, gains[1:2, :])
    hidden = jnp.dot(again, up_weight[...], preferred_element_type=jnp.float32)
    hidden = (0.5 * hidden * (1.0 + lax.erf(hidden * 0.7071067811865476))).astype(jnp.bfloat16)
    result = after + jnp.dot(hidden, down_weight[...], preferred_element_type=jnp.float32)
    result = result.astype(jnp.bfloat16).reshape(mesh_blocks, rows, width)
    for m in range(mesh_blocks):
        store_part(m, mesh_blocks, even[0], result[m], head, tail, edge)


def part_shapes(count, rows, width):
    return [
        jax.ShapeDtypeStruct((size, rows, width), jnp.bfloat16) for size in (count - 1, 1, 1)
    ]


def any_specs(count):
    return [pl.BlockSpec(memory_space=pl.ANY)] * count


VMEM_SPEC = pl.BlockSpec(memory_space=pltpu.MemorySpace.VMEM)


def shards(
    grid_feats, lift_index, lift_weight, window_index, window_count, norm_gains,
    qkv_weight, out_weight, up_weight, down_weight, return_index, return_weight,
):
    even_sector = lax.axis_index("lon") % 2 == 0
    lon_count = lax.axis_size("lon")
    grid_blocks = grid_feats.shape[1]
    mesh_blocks = lift_index.shape[1]
    rows, width = grid_feats.shape[2:]
    grid_lon = grid_blocks * lon_count
    mesh_lon = mesh_blocks * lon_count
    bf16, f32 = jnp.bfloat16, jnp.float32
    mesh_table = 3 * mesh_blocks + 6
    grid_table = 3 * grid_blocks + 6

    own_grid = grid_feats[0]
    sent = (own_grid * GRID_SCALE).astype(jnp.float16)
    sent_edge = (jnp.where(even_sector, own_grid[:1], own_grid[-1:]) * GRID_SCALE).astype(jnp.float16)
    even = even_sector.astype(jnp.int32).reshape(1)
    near, far, outer, inner = exchange((sent[:-1], sent[-1:]), sent_edge, even_sector)
    grid_pieces = [own_grid] + [
        piece.astype(f32) * (1.0 / GRID_SCALE) for piece in near + far + outer + inner
    ]
    lift_slots = table_slots(lift_index[0], grid_lon, grid_blocks).reshape(-1)
    picks = lift_weight.shape[2]
    mesh_in, normed, head, tail, edge = pl.pallas_call(
        lambda *refs: lift_kernel(*refs, piece_count=len(grid_pieces)),
        grid_spec=pltpu.PrefetchScalarGridSpec(
            num_scalar_prefetch=2,
            in_specs=any_specs(len(grid_pieces)) + [VMEM_SPEC, VMEM_SPEC],
            out_specs=[VMEM_SPEC] * 5,
            scratch_shapes=[
                pltpu.VMEM((grid_table, rows, width), f32),
                pltpu.VMEM((picks * rows, width), bf16),
                pltpu.VMEM((picks * rows, width), bf16),
                pltpu.VMEM((2 * rows, picks * rows), bf16),
                pltpu.SemaphoreType.DMA((len(grid_pieces),)),
            ],
        ),
        out_shape=[
            jax.ShapeDtypeStruct((mesh_blocks, rows, width), f32),
            jax.ShapeDtypeStruct((mesh_blocks, rows, width), bf16),
        ] + part_shapes(mesh_blocks, rows, width),
        name="lift",
    )(lift_slots, even, *grid_pieces, lift_weight[0], norm_gains)

    near, far, outer, inner = exchange((head, tail), edge, even_sector)
    own = jnp.dot(normed.reshape(-1, width), qkv_weight, preferred_element_type=f32).astype(bf16)
    queries = own[:, :width].reshape(mesh_blocks, rows, width)
    kv_weight = qkv_weight[:, width:]
    kv_pieces = [own[:, width:].reshape(mesh_blocks, rows, 2 * width)]

    def project(group):
        stacked = jnp.concatenate(group, axis=0) if len(group) > 1 else group[0]
        return (
            jnp.dot(stacked.reshape(-1, width), kv_weight, preferred_element_type=f32)
            .astype(bf16)
            .reshape(-1, rows, 2 * width)
        )

    kv_pieces.append(project(near))
    side = project(outer + inner[:1])
    kv_pieces.append(project(far))
    kv_pieces.append(side)
    kv_pieces.append(project(inner[1:]))
    window_slots = table_slots(window_index[0], mesh_lon, mesh_blocks).reshape(-1)
    neighbours = window_index.shape[2]
    hidden_width = up_weight.shape[1]
    head, tail, edge = pl.pallas_call(
        lambda *refs: layer_kernel(*refs, piece_count=len(kv_pieces)),
        grid_spec=pltpu.PrefetchScalarGridSpec(
            num_scalar_prefetch=3,
            in_specs=any_specs(len(kv_pieces)) + [VMEM_SPEC] * 3 + any_specs(3),
            out_specs=[VMEM_SPEC] * 3,
            scratch_shapes=[
                pltpu.VMEM((mesh_table, rows, 2 * width), bf16),
                pltpu.VMEM((neighbours * rows, width), bf16),
                pltpu.VMEM((HEADS // 2, neighbours * rows, 4 * (width // HEADS)), bf16),
                pltpu.VMEM((mesh_blocks * rows, width), bf16),
                pltpu.VMEM((width, width), bf16),
                pltpu.VMEM((width, hidden_width), bf16),
                pltpu.VMEM((hidden_width, width), bf16),
                pltpu.SemaphoreType.DMA((len(kv_pieces) + 3,)),
            ],
        ),
        out_shape=part_shapes(mesh_blocks, rows, width),
        name="layer",
    )(
        window_slots, window_count[0], even, *kv_pieces, queries, mesh_in, norm_gains,
        out_weight, up_weight, down_weight,
    )

    near, far, outer, inner = exchange((head, tail), edge, even_sector)
    mesh_pieces = [head, tail] + near + far + outer + inner
    return_slots = table_slots(return_index[0], mesh_lon, mesh_blocks).reshape(-1)
    grid_out = pl.pallas_call(
        lambda *refs: return_kernel(*refs, piece_count=len(mesh_pieces)),
        grid_spec=pltpu.PrefetchScalarGridSpec(
            num_scalar_prefetch=1,
            in_specs=any_specs(len(mesh_pieces)) + [VMEM_SPEC],
            out_specs=VMEM_SPEC,
            scratch_shapes=[
                pltpu.VMEM((mesh_table, rows, width), bf16),
                pltpu.VMEM((picks * rows, width), bf16),
                pltpu.VMEM((2 * rows, picks * rows), bf16),
                pltpu.SemaphoreType.DMA((len(mesh_pieces),)),
            ],
        ),
        out_shape=jax.ShapeDtypeStruct((grid_blocks, rows, width), f32),
        name="give_back",
    )(return_slots, *mesh_pieces, return_weight[0])
    return grid_out.reshape(1, grid_blocks, rows, width)


def solution(mesh):
    placed = (
        P("lat", "lon", None, None),
        P("lat", "lon", None),
        P("lat", "lon", None, None, None),
        P("lat", "lon", None),
        P("lat", "lon"),
        P(),
        P(),
        P(),
        P(),
        P(),
        P("lat", "lon", None),
        P("lat", "lon", None, None, None),
    )

    return jax.shard_map(shards, mesh=mesh, in_specs=placed, out_specs=P("lat", "lon", None, None), check_vma=False)
```

```python
import jax
import jax.numpy as jnp
from jax import lax
from jax.experimental import pallas as pl
from jax.experimental.pallas import tpu as pltpu
from jax.sharding import PartitionSpec as P


HEADS = 16
EPSILON = 1e-05
AXES = ("lat", "lon")
GRID_SCALE = 8192.0


def relay_band(band):
    return band + 2 if band % 2 == 0 else band - 2


def outer_sector(sector):
    return sector - 1 if sector % 2 == 0 else sector + 1


def move(values, band_of, sector_of):
    bands, sectors = lax.axis_size("lat"), lax.axis_size("lon")
    pairs = []
    for band in range(bands):
        for sector in range(sectors):
            target = band_of(band)
            if 0 <= target < bands:
                pairs.append((band * sectors + sector, target * sectors + sector_of(sector) % sectors))
    return lax.ppermute(values, AXES, pairs)


def same(index):
    return index


def pair(index):
    return index ^ 1


def exchange(blocks):
    near = [move(block, pair, same) for block in blocks]
    far = [move(block, relay_band, same) for block in near]
    outer = [
        move(blocks[0], same, outer_sector),
        move(blocks[0], pair, outer_sector),
        move(far[0], same, outer_sector),
    ]
    inner = [
        move(jnp.concatenate([blocks[-1], near[-1]], axis=0), same, pair), move(far[-1], same, pair)
    ]
    return near, far, outer[:2] + inner[:1], outer[2:] + inner[1:]


def table_slots(global_ids, total_lon, blocks_here, own_in_order):
    band_here = lax.axis_index("lat")
    sector_here = lax.axis_index("lon")
    band_step = global_ids // total_lon - band_here
    column = (global_ids % total_lon - sector_here * blocks_here + 1) % total_lon
    near_step = jnp.where(band_here % 2 == 0, 1, -1)
    group = jnp.where(band_step == 0, 0, jnp.where(band_step == near_step, 1, 2))
    even = sector_here % 2 == 0
    outer_column = jnp.where(even, 0, blocks_here + 1)
    outer_first = jnp.where(even, column - 1, blocks_here - column)
    if own_in_order:
        outer_first = jnp.where(group == 0, column - 1, outer_first)
    inside = group * blocks_here + outer_first
    is_outer = column == outer_column
    outside = 3 * blocks_here + jnp.where(
        group == 2, jnp.where(is_outer, 4, 5), jnp.where(is_outer, 0, 2) + group
    )
    own_column = jnp.logical_and(column >= 1, column <= blocks_here)
    return jnp.where(own_column, inside, outside)


def fill_table(pieces, table, sems):
    copies = []
    start = 0
    for place, piece in enumerate(pieces):
        count = piece.shape[0]
        copies.append(pltpu.make_async_copy(piece, table.at[pl.ds(start, count)], sems.at[place]))
        start += count
    return copies


def normalise(values, gain):
    centred = values - jnp.mean(values, axis=-1, keepdims=True)
    spread = jnp.mean(centred * centred, axis=-1, keepdims=True)
    return (centred * lax.rsqrt(spread + EPSILON) * gain).astype(jnp.bfloat16)


def two_parts(values):
    upper = lax.reduce_precision(values, 8, 7)
    return upper.astype(jnp.bfloat16), (values - upper).astype(jnp.bfloat16)


def stacked_weights(weight):
    count, picks, rows, width = weight.shape
    wide = weight.transpose(0, 2, 1, 3).reshape(count, rows, picks * width)
    return jnp.concatenate(two_parts(wide), axis=1)


def mix_blocks(slots, place, split, table, upper, lower):
    width = table.shape[1]
    rows = split.shape[0] // 2
    for k in range(split.shape[1] // width):
        block = table[slots[place, k]]
        high = block.astype(jnp.bfloat16)
        upper[k * width:(k + 1) * width, :] = high
        if lower is not None:
            lower[k * width:(k + 1) * width, :] = (block - high.astype(jnp.float32)).astype(jnp.bfloat16)
    both = jnp.dot(split[...], upper[...], preferred_element_type=jnp.float32)
    total = both[:rows] + both[rows:]
    if lower is not None:
        total = total + jnp.dot(split[0:rows, :], lower[...], preferred_element_type=jnp.float32)
    return total


def block_at(place, count, even):
    return jnp.where(even[0] == 1, place, count - 1 - place)


def lift_kernel(slots, even, *refs, piece_count):
    pieces = refs[:piece_count]
    split, gains, mesh_in, *rest = refs[piece_count:]
    table, upper, lower, sems = rest[-4:]
    parts = rest[:-4]
    copies = fill_table(pieces, table, sems)
    for copy in copies:
        copy.start()
    for copy in copies:
        copy.wait()
    for m, part in enumerate(parts):
        source = block_at(m, len(parts), even)
        mixed = mix_blocks(slots, source, split.at[source], table, upper, lower)
        mesh_in[m] = mixed
        part[0] = normalise(mixed, gains[0:1, :])


def return_kernel(slots, *refs, piece_count):
    pieces = refs[:piece_count]
    split, out, table, upper, sems = refs[piece_count:]
    copies = fill_table(pieces, table, sems)
    for copy in copies:
        copy.start()
    for copy in copies:
        copy.wait()
    for g in range(split.shape[0]):
        out[g] = mix_blocks(slots, g, split.at[g], table, upper, None)


def layer_kernel(slots, counts, even, *refs, piece_count):
    pieces = refs[:piece_count]
    queries, mesh_in, gains, out_hbm, up_hbm, down_hbm, *rest = refs[piece_count:]
    table, keys, values, mixed, out_weight, up_weight, down_weight, sems = rest[-8:]
    parts = rest[:-8]
    copies = fill_table(pieces, table, sems)
    weights = [
        pltpu.make_async_copy(out_hbm, out_weight, sems.at[piece_count]),
        pltpu.make_async_copy(up_hbm, up_weight, sems.at[piece_count + 1]),
        pltpu.make_async_copy(down_hbm, down_weight, sems.at[piece_count + 2]),
    ]
    for copy in copies + weights:
        copy.start()
    for copy in copies:
        copy.wait()
    mesh_blocks, rows, width = mesh_in.shape
    neighbours = keys.shape[0] // rows
    head_size = width // HEADS
    wide = 2 * head_size
    certain = neighbours // 2 * rows
    low_half = lax.broadcasted_iota(jnp.int32, (rows, wide), 1) < head_size
    key_block = lax.broadcasted_iota(jnp.int32, (1, neighbours * rows - certain), 1) // rows + neighbours // 2
    values[:, :, wide:] = jnp.ones((HEADS // 2, neighbours * rows, wide), jnp.bfloat16)

    def attend(m, carry):
        source = block_at(m, mesh_blocks, even)
        for j in range(neighbours):
            slot = slots[source, j]
            keys[j * rows:(j + 1) * rows, :] = table[slot, :, 0:width]
            for h in range(HEADS // 2):
                at = width + h * wide
                values[h, j * rows:(j + 1) * rows, 0:wide] = table[slot, :, at:at + wide]
        bias = jnp.where(key_block < counts[source], 0.0, -1e30)
        for h in range(HEADS // 2):
            at = h * wide
            query = queries[m, :, at:at + wide] * jnp.asarray(head_size ** (-0.5), jnp.bfloat16)
            none = jnp.zeros_like(query)
            pair_rows = jnp.concatenate(
                [jnp.where(low_half, query, none), jnp.where(low_half, none, query)], axis=0
            )
            scores = lax.dot_general(
                pair_rows, keys[:, at:at + wide], (((1,), (1,)), ((), ())), preferred_element_type=jnp.float32
            )
            first, second = scores[:, :certain], scores[:, certain:] + bias
            highest = jnp.maximum(
                jnp.max(first, axis=-1, keepdims=True), jnp.max(second, axis=-1, keepdims=True)
            )
            raw = jnp.concatenate(
                [jnp.exp(first - highest).astype(jnp.bfloat16), jnp.exp(second - highest).astype(jnp.bfloat16)],
                axis=1,
            )
            summed = jnp.dot(raw, values[h], preferred_element_type=jnp.float32)
            part = summed[:, :wide] / summed[:, wide:]
            mixed[pl.ds(m * rows, rows), at:at + wide] = jnp.where(
                low_half, part[:rows], part[rows:]
            ).astype(jnp.bfloat16)
        return carry

    lax.fori_loop(0, mesh_blocks, attend, 0)
    for copy in weights:
        copy.wait()
    after = mesh_in[...].reshape(mesh_blocks * rows, width) + jnp.dot(
        mixed[...], out_weight[...], preferred_element_type=jnp.float32
    )
    again = normalise(after, gains[1:2, :])
    hidden = jnp.dot(again, up_weight[...], preferred_element_type=jnp.float32)
    hidden = (0.5 * hidden * (1.0 + lax.erf(hidden * 0.7071067811865476))).astype(jnp.bfloat16)
    result = after + jnp.dot(hidden, down_weight[...], preferred_element_type=jnp.float32)
    result = result.astype(jnp.bfloat16).reshape(mesh_blocks, rows, width)
    for m in range(mesh_blocks):
        parts[m][0] = result[m]


def any_specs(count):
    return [pl.BlockSpec(memory_space=pl.ANY)] * count


VMEM_SPEC = pl.BlockSpec(memory_space=pltpu.MemorySpace.VMEM)


def shards(
    grid_feats, lift_index, lift_weight, window_index, window_count, norm_gains,
    qkv_weight, out_weight, up_weight, down_weight, return_index, return_weight,
):
    even_sector = lax.axis_index("lon") % 2 == 0
    lon_count = lax.axis_size("lon")
    grid_blocks = grid_feats.shape[1]
    mesh_blocks = lift_index.shape[1]
    rows, width = grid_feats.shape[2:]
    grid_lon = grid_blocks * lon_count
    mesh_lon = mesh_blocks * lon_count
    bf16, f32 = jnp.bfloat16, jnp.float32
    mesh_table = 3 * mesh_blocks + 6
    grid_table = 3 * grid_blocks + 6

    even = even_sector.astype(jnp.int32).reshape(1)
    part_shapes = [jax.ShapeDtypeStruct((1, rows, width), bf16)] * mesh_blocks
    own_grid = grid_feats[0]
    sent = []
    for i in range(grid_blocks):
        mirror = grid_blocks - 1 - i
        chosen = jnp.where(even_sector, own_grid[i:i + 1], own_grid[mirror:mirror + 1])
        sent.append((chosen * GRID_SCALE).astype(jnp.float16))
    near, far, side, last = exchange(sent)

    def decode(pieces):
        return [piece.astype(f32) * (1.0 / GRID_SCALE) for piece in pieces]

    grid_pieces = [own_grid] + decode(near) + decode(far)
    grid_pieces += decode(side) + decode(last)
    lift_slots = table_slots(lift_index[0], grid_lon, grid_blocks, True)
    picks = lift_weight.shape[2]
    mesh_in, *parts = pl.pallas_call(
        lambda *refs: lift_kernel(*refs, piece_count=len(grid_pieces)),
        grid_spec=pltpu.PrefetchScalarGridSpec(
            num_scalar_prefetch=2,
            in_specs=any_specs(len(grid_pieces)) + [VMEM_SPEC, VMEM_SPEC],
            out_specs=[VMEM_SPEC] * (1 + mesh_blocks),
            scratch_shapes=[
                pltpu.VMEM((grid_table, rows, width), f32),
                pltpu.VMEM((picks * rows, width), bf16),
                pltpu.VMEM((picks * rows, width), bf16),
                pltpu.SemaphoreType.DMA((len(grid_pieces),)),
            ],
        ),
        out_shape=[
            jax.ShapeDtypeStruct((mesh_blocks, rows, width), f32),
        ] + part_shapes,
        name="lift",
    )(lift_slots, even, *grid_pieces, stacked_weights(lift_weight[0]), norm_gains)

    near, far, side, last = exchange(parts)
    normed = jnp.concatenate(parts, axis=0)
    own = jnp.dot(normed.reshape(-1, width), qkv_weight, preferred_element_type=f32).astype(bf16)
    queries = own[:, :width].reshape(mesh_blocks, rows, width)
    kv_weight = qkv_weight[:, width:]
    kv_pieces = [own[:, width:].reshape(mesh_blocks, rows, 2 * width)]

    def project(group):
        stacked = jnp.concatenate(group, axis=0) if len(group) > 1 else group[0]
        return (
            jnp.dot(stacked.reshape(-1, width), kv_weight, preferred_element_type=f32)
            .astype(bf16)
            .reshape(-1, rows, 2 * width)
        )

    kv_pieces.append(project(near))
    side = project(side)
    kv_pieces.append(project(far))
    kv_pieces += [side, project(last)]
    window_slots = table_slots(window_index[0], mesh_lon, mesh_blocks, False)
    neighbours = window_index.shape[2]
    hidden_width = up_weight.shape[1]
    parts = pl.pallas_call(
        lambda *refs: layer_kernel(*refs, piece_count=len(kv_pieces)),
        grid_spec=pltpu.PrefetchScalarGridSpec(
            num_scalar_prefetch=3,
            in_specs=any_specs(len(kv_pieces)) + [VMEM_SPEC] * 3 + any_specs(3),
            out_specs=[VMEM_SPEC] * mesh_blocks,
            scratch_shapes=[
                pltpu.VMEM((mesh_table, rows, 2 * width), bf16),
                pltpu.VMEM((neighbours * rows, width), bf16),
                pltpu.VMEM((HEADS // 2, neighbours * rows, 4 * (width // HEADS)), bf16),
                pltpu.VMEM((mesh_blocks * rows, width), bf16),
                pltpu.VMEM((width, width), bf16),
                pltpu.VMEM((width, hidden_width), bf16),
                pltpu.VMEM((hidden_width, width), bf16),
                pltpu.SemaphoreType.DMA((len(kv_pieces) + 3,)),
            ],
        ),
        out_shape=part_shapes,
        name="layer",
    )(
        window_slots, window_count[0], even, *kv_pieces, queries, mesh_in, norm_gains,
        out_weight, up_weight, down_weight,
    )

    near, far, side, last = exchange(parts)
    mesh_pieces = list(parts) + near + far + side + last
    return_slots = table_slots(return_index[0], mesh_lon, mesh_blocks, False)
    grid_out = pl.pallas_call(
        lambda *refs: return_kernel(*refs, piece_count=len(mesh_pieces)),
        grid_spec=pltpu.PrefetchScalarGridSpec(
            num_scalar_prefetch=1,
            in_specs=any_specs(len(mesh_pieces)) + [VMEM_SPEC],
            out_specs=VMEM_SPEC,
            scratch_shapes=[
                pltpu.VMEM((mesh_table, rows, width), bf16),
                pltpu.VMEM((picks * rows, width), bf16),
                pltpu.SemaphoreType.DMA((len(mesh_pieces),)),
            ],
        ),
        out_shape=jax.ShapeDtypeStruct((grid_blocks, rows, width), f32),
        name="give_back",
    )(return_slots, *mesh_pieces, stacked_weights(return_weight[0]))
    return grid_out.reshape(1, grid_blocks, rows, width)


def solution(mesh):
    placed = (
        P("lat", "lon", None, None),
        P("lat", "lon", None),
        P("lat", "lon", None, None, None),
        P("lat", "lon", None),
        P("lat", "lon"),
        P(),
        P(),
        P(),
        P(),
        P(),
        P("lat", "lon", None),
        P("lat", "lon", None, None, None),
    )

    return jax.shard_map(
        shards, mesh=mesh, in_specs=placed, out_specs=P("lat", "lon", None, None), check_vma=False
    )
```

```python
import jax
import jax.numpy as jnp
from jax import lax
from jax.experimental import pallas as pl
from jax.experimental.pallas import tpu as pltpu
from jax.sharding import PartitionSpec as P


HEADS = 16
EPSILON = 1e-05
AXES = ("lat", "lon")
GRID_SCALE = 8192.0
MEBI = 1024 * 1024


def relay_band(band):
    return band + 2 if band % 2 == 0 else band - 2


def outer_sector(sector):
    return sector - 1 if sector % 2 == 0 else sector + 1


def move(values, band_of, sector_of):
    bands, sectors = lax.axis_size("lat"), lax.axis_size("lon")
    pairs = []
    for band in range(bands):
        for sector in range(sectors):
            target = band_of(band)
            if 0 <= target < bands:
                pairs.append((band * sectors + sector, target * sectors + sector_of(sector) % sectors))
    return lax.ppermute(values, AXES, pairs)


def same(index):
    return index


def pair(index):
    return index ^ 1


def exchange(blocks):
    near = [move(block, pair, same) for block in blocks]
    far = [move(block, relay_band, same) for block in near]
    outer = [
        move(blocks[0], same, outer_sector),
        move(blocks[0], pair, outer_sector),
        move(far[0], same, outer_sector),
    ]
    inner = [
        move(jnp.concatenate([blocks[-1], near[-1]], axis=0), same, pair), move(far[-1], same, pair)
    ]
    return near, far, outer[:2] + inner[:1], outer[2:] + inner[1:]


def table_slots(global_ids, total_lon, blocks_here, own_in_order):
    band_here = lax.axis_index("lat")
    sector_here = lax.axis_index("lon")
    band_step = global_ids // total_lon - band_here
    column = (global_ids % total_lon - sector_here * blocks_here + 1) % total_lon
    near_step = jnp.where(band_here % 2 == 0, 1, -1)
    group = jnp.where(band_step == 0, 0, jnp.where(band_step == near_step, 1, 2))
    even = sector_here % 2 == 0
    outer_column = jnp.where(even, 0, blocks_here + 1)
    outer_first = jnp.where(even, column - 1, blocks_here - column)
    if own_in_order:
        outer_first = jnp.where(group == 0, column - 1, outer_first)
    inside = group * blocks_here + outer_first
    is_outer = column == outer_column
    outside = 3 * blocks_here + jnp.where(
        group == 2, jnp.where(is_outer, 4, 5), jnp.where(is_outer, 0, 2) + group
    )
    own_column = jnp.logical_and(column >= 1, column <= blocks_here)
    return jnp.where(own_column, inside, outside)


def fill_table(pieces, table, sems):
    copies = []
    start = 0
    for place, piece in enumerate(pieces):
        count = piece.shape[0]
        copies.append(pltpu.make_async_copy(piece, table.at[pl.ds(start, count)], sems.at[place]))
        start += count
    return copies


def normalise(values, gain):
    centred = values - jnp.mean(values, axis=-1, keepdims=True)
    spread = jnp.mean(centred * centred, axis=-1, keepdims=True)
    return (centred * lax.rsqrt(spread + EPSILON) * gain).astype(jnp.bfloat16)


def two_parts(values):
    upper = lax.reduce_precision(values, 8, 7)
    return upper.astype(jnp.bfloat16), (values - upper).astype(jnp.bfloat16)


def stacked_weights(weight):
    count, picks, rows, width = weight.shape
    wide = weight.transpose(0, 2, 1, 3).reshape(count, rows, picks * width)
    return jnp.concatenate(two_parts(wide), axis=1)


def mix_blocks(slots, place, split, table, upper, lower):
    width = table.shape[1]
    rows = split.shape[0] // 2
    for k in range(split.shape[1] // width):
        block = table[slots[place, k]]
        high = block.astype(jnp.bfloat16)
        upper[k * width:(k + 1) * width, :] = high
        if lower is not None:
            lower[k * width:(k + 1) * width, :] = (block - high.astype(jnp.float32)).astype(jnp.bfloat16)
    both = jnp.dot(split[...], upper[...], preferred_element_type=jnp.float32)
    total = both[:rows] + both[rows:]
    if lower is not None:
        total = total + jnp.dot(split[0:rows, :], lower[...], preferred_element_type=jnp.float32)
    return total


def block_at(place, count, even):
    return jnp.where(even[0] == 1, place, count - 1 - place)


def lift_kernel(slots, even, *refs, piece_count):
    pieces = refs[:piece_count]
    split, gains, mesh_in, *rest = refs[piece_count:]
    table, upper, lower, sems = rest[-4:]
    parts = rest[:-4]
    copies = fill_table(pieces, table, sems)
    for copy in copies:
        copy.start()
    for copy in copies:
        copy.wait()
    for m, part in enumerate(parts):
        source = block_at(m, len(parts), even)
        mixed = mix_blocks(slots, source, split.at[source], table, upper, lower)
        mesh_in[m] = mixed
        part[0] = normalise(mixed, gains[0:1, :])


def return_kernel(slots, *refs, piece_count):
    pieces = refs[:piece_count]
    split, out, table, upper, sems = refs[piece_count:]
    copies = fill_table(pieces, table, sems)
    for copy in copies:
        copy.start()
    for copy in copies:
        copy.wait()
    for g in range(split.shape[0]):
        out[g] = mix_blocks(slots, g, split.at[g], table, upper, None)


def layer_kernel(slots, counts, even, *refs, piece_count):
    pieces = refs[:piece_count]
    queries, mesh_in, gains, out_hbm, up_hbm, down_hbm, *rest = refs[piece_count:]
    table, keys, values, mixed, out_weight, up_weight, down_weight, sems = rest[-8:]
    parts = rest[:-8]
    copies = fill_table(pieces, table, sems)
    weights = [
        pltpu.make_async_copy(out_hbm, out_weight, sems.at[piece_count]),
        pltpu.make_async_copy(up_hbm, up_weight, sems.at[piece_count + 1]),
        pltpu.make_async_copy(down_hbm, down_weight, sems.at[piece_count + 2]),
    ]
    for copy in copies + weights:
        copy.start()
    for copy in copies:
        copy.wait()
    mesh_blocks, rows, width = mesh_in.shape
    neighbours = keys.shape[0] // rows
    head_size = width // HEADS
    wide = 2 * head_size
    certain = neighbours // 2 * rows
    low_half = lax.broadcasted_iota(jnp.int32, (rows, wide), 1) < head_size
    key_block = lax.broadcasted_iota(jnp.int32, (1, neighbours * rows - certain), 1) // rows + neighbours // 2
    values[:, :, wide:] = jnp.ones((HEADS // 2, neighbours * rows, wide), jnp.bfloat16)

    def attend(m, carry):
        source = block_at(m, mesh_blocks, even)
        for j in range(neighbours):
            slot = slots[source, j]
            keys[j * rows:(j + 1) * rows, :] = table[slot, :, 0:width]
            for h in range(HEADS // 2):
                at = width + h * wide
                values[h, j * rows:(j + 1) * rows, 0:wide] = table[slot, :, at:at + wide]
        bias = jnp.where(key_block < counts[source], 0.0, -1e30)

        def score(h):
            at = h * wide
            query = queries[m, :, at:at + wide] * jnp.asarray(head_size ** (-0.5), jnp.bfloat16)
            none = jnp.zeros_like(query)
            pair_rows = jnp.concatenate(
                [jnp.where(low_half, query, none), jnp.where(low_half, none, query)], axis=0
            )
            return lax.dot_general(
                pair_rows, keys[:, at:at + wide], (((1,), (1,)), ((), ())), preferred_element_type=jnp.float32
            )

        following = score(0)
        for h in range(HEADS // 2):
            at = h * wide
            scores = following
            if h + 1 < HEADS // 2:
                following = score(h + 1)
            first, second = scores[:, :certain], scores[:, certain:] + bias
            highest = jnp.maximum(
                jnp.max(first, axis=-1, keepdims=True), jnp.max(second, axis=-1, keepdims=True)
            )
            raw = jnp.concatenate(
                [jnp.exp(first - highest).astype(jnp.bfloat16), jnp.exp(second - highest).astype(jnp.bfloat16)],
                axis=1,
            )
            summed = jnp.dot(raw, values[h], preferred_element_type=jnp.float32)
            part = summed[:, :wide] / summed[:, wide:]
            mixed[pl.ds(m * rows, rows), at:at + wide] = jnp.where(
                low_half, part[:rows], part[rows:]
            ).astype(jnp.bfloat16)
        return carry

    lax.fori_loop(0, mesh_blocks, attend, 0)
    for copy in weights:
        copy.wait()
    after = mesh_in[...].reshape(mesh_blocks * rows, width) + jnp.dot(
        mixed[...], out_weight[...], preferred_element_type=jnp.float32
    )
    again = normalise(after, gains[1:2, :])
    hidden = jnp.dot(again, up_weight[...], preferred_element_type=jnp.float32)
    hidden = (0.5 * hidden * (1.0 + lax.erf(hidden * 0.7071067811865476))).astype(jnp.bfloat16)
    result = after + jnp.dot(hidden, down_weight[...], preferred_element_type=jnp.float32)
    result = result.astype(jnp.bfloat16).reshape(mesh_blocks, rows, width)
    for m in range(mesh_blocks):
        parts[m][0] = result[m]


def any_specs(count):
    return [pl.BlockSpec(memory_space=pl.ANY)] * count


VMEM_SPEC = pl.BlockSpec(memory_space=pltpu.MemorySpace.VMEM)


def shards(
    grid_feats, lift_index, lift_weight, window_index, window_count, norm_gains,
    qkv_weight, out_weight, up_weight, down_weight, return_index, return_weight,
):
    even_sector = lax.axis_index("lon") % 2 == 0
    lon_count = lax.axis_size("lon")
    grid_blocks = grid_feats.shape[1]
    mesh_blocks = lift_index.shape[1]
    rows, width = grid_feats.shape[2:]
    grid_lon = grid_blocks * lon_count
    mesh_lon = mesh_blocks * lon_count
    bf16, f32 = jnp.bfloat16, jnp.float32
    mesh_table = 3 * mesh_blocks + 6
    grid_table = 3 * grid_blocks + 6

    even = even_sector.astype(jnp.int32).reshape(1)
    part_shapes = [jax.ShapeDtypeStruct((1, rows, width), bf16)] * mesh_blocks
    own_grid = grid_feats[0]
    sent = []
    for i in range(grid_blocks):
        mirror = grid_blocks - 1 - i
        chosen = jnp.where(even_sector, own_grid[i:i + 1], own_grid[mirror:mirror + 1])
        sent.append((chosen * GRID_SCALE).astype(jnp.float16))
    near, far, side, last = exchange(sent)

    def decode(pieces):
        return [piece.astype(f32) * (1.0 / GRID_SCALE) for piece in pieces]

    grid_pieces = [own_grid] + decode(near) + decode(far)
    grid_pieces += decode(side) + decode(last)
    lift_slots = table_slots(lift_index[0], grid_lon, grid_blocks, True)
    picks = lift_weight.shape[2]
    mesh_in, *parts = pl.pallas_call(
        lambda *refs: lift_kernel(*refs, piece_count=len(grid_pieces)),
        grid_spec=pltpu.PrefetchScalarGridSpec(
            num_scalar_prefetch=2,
            in_specs=any_specs(len(grid_pieces)) + [VMEM_SPEC, VMEM_SPEC],
            out_specs=[VMEM_SPEC] * (1 + mesh_blocks),
            scratch_shapes=[
                pltpu.VMEM((grid_table, rows, width), f32),
                pltpu.VMEM((picks * rows, width), bf16),
                pltpu.VMEM((picks * rows, width), bf16),
                pltpu.SemaphoreType.DMA((len(grid_pieces),)),
            ],
        ),
        out_shape=[
            jax.ShapeDtypeStruct((mesh_blocks, rows, width), f32),
        ] + part_shapes,
        compiler_params=pltpu.CompilerParams(vmem_limit_bytes=20 * MEBI),
        name="lift",
    )(lift_slots, even, *grid_pieces, stacked_weights(lift_weight[0]), norm_gains)

    near, far, side, last = exchange(parts)
    normed = jnp.concatenate(parts, axis=0)
    own = jnp.dot(normed.reshape(-1, width), qkv_weight, preferred_element_type=f32).astype(bf16)
    queries = own[:, :width].reshape(mesh_blocks, rows, width)
    kv_weight = qkv_weight[:, width:]
    kv_pieces = [own[:, width:].reshape(mesh_blocks, rows, 2 * width)]

    def project(group):
        stacked = jnp.concatenate(group, axis=0) if len(group) > 1 else group[0]
        return (
            jnp.dot(stacked.reshape(-1, width), kv_weight, preferred_element_type=f32)
            .astype(bf16)
            .reshape(-1, rows, 2 * width)
        )

    kv_pieces.append(project(near))
    side = project(side)
    kv_pieces.append(project(far))
    kv_pieces += [side, project(last)]
    window_slots = table_slots(window_index[0], mesh_lon, mesh_blocks, False)
    neighbours = window_index.shape[2]
    hidden_width = up_weight.shape[1]
    parts = pl.pallas_call(
        lambda *refs: layer_kernel(*refs, piece_count=len(kv_pieces)),
        grid_spec=pltpu.PrefetchScalarGridSpec(
            num_scalar_prefetch=3,
            in_specs=any_specs(len(kv_pieces)) + [VMEM_SPEC] * 3 + any_specs(3),
            out_specs=[VMEM_SPEC] * mesh_blocks,
            scratch_shapes=[
                pltpu.VMEM((mesh_table, rows, 2 * width), bf16),
                pltpu.VMEM((neighbours * rows, width), bf16),
                pltpu.VMEM((HEADS // 2, neighbours * rows, 4 * (width // HEADS)), bf16),
                pltpu.VMEM((mesh_blocks * rows, width), bf16),
                pltpu.VMEM((width, width), bf16),
                pltpu.VMEM((width, hidden_width), bf16),
                pltpu.VMEM((hidden_width, width), bf16),
                pltpu.SemaphoreType.DMA((len(kv_pieces) + 3,)),
            ],
        ),
        out_shape=part_shapes,
        compiler_params=pltpu.CompilerParams(vmem_limit_bytes=42 * MEBI),
        name="layer",
    )(
        window_slots, window_count[0], even, *kv_pieces, queries, mesh_in, norm_gains,
        out_weight, up_weight, down_weight,
    )

    near, far, side, last = exchange(parts)
    mesh_pieces = list(parts) + near + far + side + last
    return_slots = table_slots(return_index[0], mesh_lon, mesh_blocks, False)
    grid_out = pl.pallas_call(
        lambda *refs: return_kernel(*refs, piece_count=len(mesh_pieces)),
        grid_spec=pltpu.PrefetchScalarGridSpec(
            num_scalar_prefetch=1,
            in_specs=any_specs(len(mesh_pieces)) + [VMEM_SPEC],
            out_specs=VMEM_SPEC,
            scratch_shapes=[
                pltpu.VMEM((mesh_table, rows, width), bf16),
                pltpu.VMEM((picks * rows, width), bf16),
                pltpu.SemaphoreType.DMA((len(mesh_pieces),)),
            ],
        ),
        out_shape=jax.ShapeDtypeStruct((grid_blocks, rows, width), f32),
        compiler_params=pltpu.CompilerParams(vmem_limit_bytes=16 * MEBI),
        name="give_back",
    )(return_slots, *mesh_pieces, stacked_weights(return_weight[0]))
    return grid_out.reshape(1, grid_blocks, rows, width)


def solution(mesh):
    placed = (
        P("lat", "lon", None, None),
        P("lat", "lon", None),
        P("lat", "lon", None, None, None),
        P("lat", "lon", None),
        P("lat", "lon"),
        P(),
        P(),
        P(),
        P(),
        P(),
        P("lat", "lon", None),
        P("lat", "lon", None, None, None),
    )

    return jax.shard_map(
        shards, mesh=mesh, in_specs=placed, out_specs=P("lat", "lon", None, None), check_vma=False
    )
```

```python
import jax
import jax.numpy as jnp
from jax import lax
from jax.experimental import pallas as pl
from jax.experimental.pallas import tpu as pltpu
from jax.sharding import PartitionSpec as P


HEADS = 16
EPSILON = 1e-05
AXES = ("lat", "lon")
GRID_SCALE = 8192.0
MEBI = 1024 * 1024


def relay_band(band):
    return band + 2 if band % 2 == 0 else band - 2


def outer_sector(sector):
    return sector - 1 if sector % 2 == 0 else sector + 1


def move(values, band_of, sector_of):
    bands, sectors = lax.axis_size("lat"), lax.axis_size("lon")
    pairs = []
    for band in range(bands):
        for sector in range(sectors):
            target = band_of(band)
            if 0 <= target < bands:
                pairs.append((band * sectors + sector, target * sectors + sector_of(sector) % sectors))
    return lax.ppermute(values, AXES, pairs)


def same(index):
    return index


def pair(index):
    return index ^ 1


def exchange(blocks):
    near = [move(block, pair, same) for block in blocks]
    far = [move(block, relay_band, same) for block in near]
    outer = [move(blocks[0], same, outer_sector), move(blocks[0], pair, outer_sector), move(far[0], same, outer_sector)]
    inner = [move(jnp.concatenate([blocks[1], near[1]], axis=0), same, pair), move(far[1], same, pair)]
    return near, far, outer[:2] + inner[:1], outer[2:] + inner[1:]


def table_slots(global_ids, total_lon, blocks_here, own_in_order):
    band_here = lax.axis_index("lat")
    sector_here = lax.axis_index("lon")
    band_step = global_ids // total_lon - band_here
    column = (global_ids % total_lon - sector_here * blocks_here + 1) % total_lon
    near_step = jnp.where(band_here % 2 == 0, 1, -1)
    group = jnp.where(band_step == 0, 0, jnp.where(band_step == near_step, 1, 2))
    even = sector_here % 2 == 0
    outer_column = jnp.where(even, 0, blocks_here + 1)
    inner_column = jnp.where(even, blocks_here, 1)
    at_outer = column == jnp.where(even, 1, blocks_here)
    outer_first = jnp.where(at_outer, 0, jnp.where(column == inner_column, 1, column))
    if own_in_order:
        outer_first = jnp.where(group == 0, column - 1, outer_first)
    inside = group * blocks_here + outer_first
    is_outer = column == outer_column
    outside = 3 * blocks_here + jnp.where(
        group == 2, jnp.where(is_outer, 4, 5), jnp.where(is_outer, 0, 2) + group
    )
    own_column = jnp.logical_and(column >= 1, column <= blocks_here)
    return jnp.where(own_column, inside, outside)


def fill_table(pieces, table, sems):
    copies = []
    start = 0
    for place, piece in enumerate(pieces):
        count = piece.shape[0]
        copies.append(pltpu.make_async_copy(piece, table.at[pl.ds(start, count)], sems.at[place]))
        start += count
    return copies


def normalise(values, gain):
    centred = values - jnp.mean(values, axis=-1, keepdims=True)
    spread = jnp.mean(centred * centred, axis=-1, keepdims=True)
    return (centred * lax.rsqrt(spread + EPSILON) * gain).astype(jnp.bfloat16)


def two_parts(values):
    upper = lax.reduce_precision(values, 8, 7)
    return upper.astype(jnp.bfloat16), (values - upper).astype(jnp.bfloat16)


def stacked_weights(weight):
    count, picks, rows, width = weight.shape
    wide = weight.transpose(0, 2, 1, 3).reshape(count, rows, picks * width)
    return jnp.concatenate(two_parts(wide), axis=1)


def mix_blocks(slots, place, split, table, upper, lower):
    width = table.shape[1]
    rows = split.shape[0] // 2
    for k in range(split.shape[1] // width):
        block = table[slots[place, k]]
        high = block.astype(jnp.bfloat16)
        upper[k * width:(k + 1) * width, :] = high
        if lower is not None:
            lower[k * width:(k + 1) * width, :] = (block - high.astype(jnp.float32)).astype(jnp.bfloat16)
    both = jnp.dot(split[...], upper[...], preferred_element_type=jnp.float32)
    total = both[:rows] + both[rows:]
    if lower is not None:
        total = total + jnp.dot(split[0:rows, :], lower[...], preferred_element_type=jnp.float32)
    return total


def block_at(place, count, even):
    first = jnp.where(even[0] == 1, 0, count - 1)
    return jnp.where(place == 0, first, jnp.where(place == 1, count - 1 - first, place - 1))


def lift_kernel(slots, even, *refs, piece_count):
    pieces = refs[:piece_count]
    split, gains, mesh_in, *rest = refs[piece_count:]
    table, upper, lower, sems = rest[-4:]
    parts = rest[:-4]
    copies = fill_table(pieces, table, sems)
    for copy in copies:
        copy.start()
    for copy in copies:
        copy.wait()
    for m, part in enumerate(parts):
        source = block_at(m, len(parts), even)
        mixed = mix_blocks(slots, source, split.at[source], table, upper, lower)
        mesh_in[m] = mixed
        part[0] = normalise(mixed, gains[0:1, :])


def return_kernel(slots, *refs, piece_count):
    pieces = refs[:piece_count]
    split, out, table, upper, sems = refs[piece_count:]
    copies = fill_table(pieces, table, sems)
    for copy in copies:
        copy.start()
    for copy in copies:
        copy.wait()
    for g in range(split.shape[0]):
        out[g] = mix_blocks(slots, g, split.at[g], table, upper, None)


def layer_kernel(slots, counts, even, *refs, piece_count):
    pieces = refs[:piece_count]
    queries, mesh_in, gains, out_hbm, up_hbm, down_hbm, *rest = refs[piece_count:]
    window, mixed, out_weight, up_weight, down_weight, sems, window_sems = rest[-7:]
    parts = rest[:-7]
    mesh_blocks, rows, width = mesh_in.shape
    neighbours = window.shape[1] // rows

    def place(slot, j):
        return window.at[slot, pl.ds(j * rows, rows)]

    def fetch(m, buffer):
        source = block_at(m, mesh_blocks, even)
        for j in range(neighbours):
            slot = slots[source, j]
            start = 0
            for piece in pieces:
                count = piece.shape[0]

                @pl.when(jnp.logical_and(slot >= start, slot < start + count))
                def _(piece=piece, start=start):
                    pltpu.make_async_copy(
                        piece.at[slot - start], place(buffer, j), window_sems.at[buffer, j]
                    ).start()

                start += count

    fetch(0, 0)
    weights = [
        pltpu.make_async_copy(out_hbm, out_weight, sems.at[0]),
        pltpu.make_async_copy(up_hbm, up_weight, sems.at[1]),
        pltpu.make_async_copy(down_hbm, down_weight, sems.at[2]),
    ]
    for copy in weights:
        copy.start()
    head_size = width // HEADS
    wide = 2 * head_size
    certain = neighbours // 2 * rows
    low_half = lax.broadcasted_iota(jnp.int32, (rows, wide), 1) < head_size
    key_block = lax.broadcasted_iota(jnp.int32, (1, neighbours * rows - certain), 1) // rows + neighbours // 2
    ones = jnp.ones((neighbours * rows, wide), jnp.bfloat16)

    def attend(m, carry):
        source = block_at(m, mesh_blocks, even)
        buffer = lax.rem(m, 2)
        for j in range(neighbours):
            pltpu.make_async_copy(pieces[0].at[0], place(buffer, j), window_sems.at[buffer, j]).wait()

        @pl.when(m + 1 < mesh_blocks)
        def _():
            fetch(m + 1, 1 - buffer)

        bias = jnp.where(key_block < counts[source], 0.0, -1e30)

        def score(h):
            at = h * wide
            query = queries[m, :, at:at + wide] * jnp.asarray(head_size ** (-0.5), jnp.bfloat16)
            none = jnp.zeros_like(query)
            pair_rows = jnp.concatenate(
                [jnp.where(low_half, query, none), jnp.where(low_half, none, query)], axis=0
            )
            return lax.dot_general(
                pair_rows, window[buffer, :, at:at + wide], (((1,), (1,)), ((), ())), preferred_element_type=jnp.float32
            )

        following = score(0)
        for h in range(HEADS // 2):
            at = h * wide
            scores = following
            if h + 1 < HEADS // 2:
                following = score(h + 1)
            first, second = scores[:, :certain], scores[:, certain:] + bias
            highest = jnp.maximum(
                jnp.max(first, axis=-1, keepdims=True), jnp.max(second, axis=-1, keepdims=True)
            )
            raw = jnp.concatenate(
                [jnp.exp(first - highest).astype(jnp.bfloat16), jnp.exp(second - highest).astype(jnp.bfloat16)],
                axis=1,
            )
            columns = jnp.concatenate([window[buffer, :, width + at:width + at + wide], ones], axis=1)
            summed = jnp.dot(raw, columns, preferred_element_type=jnp.float32)
            part = summed[:, :wide] / summed[:, wide:]
            mixed[pl.ds(m * rows, rows), at:at + wide] = jnp.where(
                low_half, part[:rows], part[rows:]
            ).astype(jnp.bfloat16)
        return carry

    lax.fori_loop(0, mesh_blocks, attend, 0)
    for copy in weights:
        copy.wait()
    after = mesh_in[...].reshape(mesh_blocks * rows, width) + jnp.dot(
        mixed[...], out_weight[...], preferred_element_type=jnp.float32
    )
    again = normalise(after, gains[1:2, :])
    hidden = jnp.dot(again, up_weight[...], preferred_element_type=jnp.float32)
    hidden = (0.5 * hidden * (1.0 + lax.erf(hidden * 0.7071067811865476))).astype(jnp.bfloat16)
    result = after + jnp.dot(hidden, down_weight[...], preferred_element_type=jnp.float32)
    result = result.astype(jnp.bfloat16).reshape(mesh_blocks, rows, width)
    for m in range(mesh_blocks):
        parts[m][0] = result[m]


def any_specs(count):
    return [pl.BlockSpec(memory_space=pl.ANY)] * count


VMEM_SPEC = pl.BlockSpec(memory_space=pltpu.MemorySpace.VMEM)


def shards(
    grid_feats, lift_index, lift_weight, window_index, window_count, norm_gains,
    qkv_weight, out_weight, up_weight, down_weight, return_index, return_weight,
):
    even_sector = lax.axis_index("lon") % 2 == 0
    lon_count = lax.axis_size("lon")
    grid_blocks = grid_feats.shape[1]
    mesh_blocks = lift_index.shape[1]
    rows, width = grid_feats.shape[2:]
    grid_lon = grid_blocks * lon_count
    mesh_lon = mesh_blocks * lon_count
    bf16, f32 = jnp.bfloat16, jnp.float32
    mesh_table = 3 * mesh_blocks + 6
    grid_table = 3 * grid_blocks + 6

    even = even_sector.astype(jnp.int32).reshape(1)
    part_shapes = [jax.ShapeDtypeStruct((1, rows, width), bf16)] * mesh_blocks
    own_grid = grid_feats[0]
    sent = []
    for i in range(grid_blocks):
        mirror = grid_blocks - 1 - i
        chosen = jnp.where(even_sector, own_grid[i:i + 1], own_grid[mirror:mirror + 1])
        sent.append((chosen * GRID_SCALE).astype(jnp.float16))
    near, far, side, last = exchange(sent)

    def decode(pieces):
        return [piece.astype(f32) * (1.0 / GRID_SCALE) for piece in pieces]

    grid_pieces = [own_grid] + decode(near) + decode(far)
    grid_pieces += decode(side) + decode(last)
    lift_slots = table_slots(lift_index[0], grid_lon, grid_blocks, True)
    picks = lift_weight.shape[2]
    mesh_in, *parts = pl.pallas_call(
        lambda *refs: lift_kernel(*refs, piece_count=len(grid_pieces)),
        grid_spec=pltpu.PrefetchScalarGridSpec(
            num_scalar_prefetch=2,
            in_specs=any_specs(len(grid_pieces)) + [VMEM_SPEC, VMEM_SPEC],
            out_specs=[VMEM_SPEC] * (1 + mesh_blocks),
            scratch_shapes=[
                pltpu.VMEM((grid_table, rows, width), f32),
                pltpu.VMEM((picks * rows, width), bf16),
                pltpu.VMEM((picks * rows, width), bf16),
                pltpu.SemaphoreType.DMA((len(grid_pieces),)),
            ],
        ),
        out_shape=[
            jax.ShapeDtypeStruct((mesh_blocks, rows, width), f32),
        ] + part_shapes,
        compiler_params=pltpu.CompilerParams(vmem_limit_bytes=20 * MEBI),
        name="lift",
    )(lift_slots, even, *grid_pieces, stacked_weights(lift_weight[0]), norm_gains)

    near, far, side, last = exchange(parts)
    normed = jnp.concatenate(parts, axis=0)
    own = jnp.dot(normed.reshape(-1, width), qkv_weight, preferred_element_type=f32).astype(bf16)
    queries = own[:, :width].reshape(mesh_blocks, rows, width)
    kv_weight = qkv_weight[:, width:]
    kv_pieces = [own[:, width:].reshape(mesh_blocks, rows, 2 * width)]

    def project(group):
        stacked = jnp.concatenate(group, axis=0) if len(group) > 1 else group[0]
        return (
            jnp.dot(stacked.reshape(-1, width), kv_weight, preferred_element_type=f32)
            .astype(bf16)
            .reshape(-1, rows, 2 * width)
        )

    kv_pieces.append(project(near))
    side = project(side)
    kv_pieces.append(project(far))
    kv_pieces += [side, project(last)]
    window_slots = table_slots(window_index[0], mesh_lon, mesh_blocks, False)
    neighbours = window_index.shape[2]
    hidden_width = up_weight.shape[1]
    parts = pl.pallas_call(
        lambda *refs: layer_kernel(*refs, piece_count=len(kv_pieces)),
        grid_spec=pltpu.PrefetchScalarGridSpec(
            num_scalar_prefetch=3,
            in_specs=any_specs(len(kv_pieces)) + [VMEM_SPEC] * 3 + any_specs(3),
            out_specs=[VMEM_SPEC] * mesh_blocks,
            scratch_shapes=[
                pltpu.VMEM((2, neighbours * rows, 2 * width), bf16),
                pltpu.VMEM((mesh_blocks * rows, width), bf16),
                pltpu.VMEM((width, width), bf16),
                pltpu.VMEM((width, hidden_width), bf16),
                pltpu.VMEM((hidden_width, width), bf16),
                pltpu.SemaphoreType.DMA((3,)),
                pltpu.SemaphoreType.DMA((2, neighbours)),
            ],
        ),
        out_shape=part_shapes,
        compiler_params=pltpu.CompilerParams(vmem_limit_bytes=42 * MEBI),
        name="layer",
    )(
        window_slots, window_count[0], even, *kv_pieces, queries, mesh_in, norm_gains,
        out_weight, up_weight, down_weight,
    )

    near, far, side, last = exchange(parts)
    mesh_pieces = list(parts) + near + far + side + last
    return_slots = table_slots(return_index[0], mesh_lon, mesh_blocks, False)
    grid_out = pl.pallas_call(
        lambda *refs: return_kernel(*refs, piece_count=len(mesh_pieces)),
        grid_spec=pltpu.PrefetchScalarGridSpec(
            num_scalar_prefetch=1,
            in_specs=any_specs(len(mesh_pieces)) + [VMEM_SPEC],
            out_specs=VMEM_SPEC,
            scratch_shapes=[
                pltpu.VMEM((mesh_table, rows, width), bf16),
                pltpu.VMEM((picks * rows, width), bf16),
                pltpu.SemaphoreType.DMA((len(mesh_pieces),)),
            ],
        ),
        out_shape=jax.ShapeDtypeStruct((grid_blocks, rows, width), f32),
        compiler_params=pltpu.CompilerParams(vmem_limit_bytes=16 * MEBI),
        name="give_back",
    )(return_slots, *mesh_pieces, stacked_weights(return_weight[0]))
    return grid_out.reshape(1, grid_blocks, rows, width)


def solution(mesh):
    placed = (
        P("lat", "lon", None, None),
        P("lat", "lon", None),
        P("lat", "lon", None, None, None),
        P("lat", "lon", None),
        P("lat", "lon"),
        P(),
        P(),
        P(),
        P(),
        P(),
        P("lat", "lon", None),
        P("lat", "lon", None, None, None),
    )

    return jax.shard_map(shards, mesh=mesh, in_specs=placed, out_specs=P("lat", "lon", None, None), check_vma=False)
```

```python
import jax
import jax.numpy as jnp
from jax import lax
from jax.experimental import pallas as pl
from jax.experimental.pallas import tpu as pltpu
from jax.sharding import PartitionSpec as P


HEADS = 16
EPSILON = 1e-05
AXES = ("lat", "lon")
GRID_SCALE = 8192.0
MEBI = 1024 * 1024


def far_band(band):
    return band - 1 if band % 2 == 0 else band + 1


def relay_band(band):
    return band + 2 if band % 2 == 0 else band - 2


def outer_sector(sector):
    return sector - 1 if sector % 2 == 0 else sector + 1


def move(values, band_of, sector_of):
    bands, sectors = lax.axis_size("lat"), lax.axis_size("lon")
    pairs = []
    for band in range(bands):
        for sector in range(sectors):
            target = band_of(band)
            if 0 <= target < bands:
                pairs.append((band * sectors + sector, target * sectors + sector_of(sector) % sectors))
    return lax.ppermute(values, AXES, pairs)


def same(index):
    return index


def pair(index):
    return index ^ 1


def exchange(blocks):
    half = blocks[0].shape[1] // 2
    near = [move(block, pair, same) for block in blocks]
    far = [move(block, relay_band, same) for block in near]
    outer = [
        move(blocks[0], same, outer_sector),
        move(blocks[0], pair, outer_sector),
        jnp.concatenate(
            [
                move(far[0][:, :half], same, outer_sector),
                move(blocks[0][:, half:], far_band, outer_sector),
            ],
            axis=1,
        ),
    ]
    inner = [
        move(jnp.concatenate([blocks[1], near[1]], axis=0), same, pair), move(far[1], same, pair)
    ]
    return near, far, outer[:2] + inner[:1], outer[2:] + inner[1:]


def table_slots(global_ids, total_lon, blocks_here, own_in_order):
    band_here = lax.axis_index("lat")
    sector_here = lax.axis_index("lon")
    band_step = global_ids // total_lon - band_here
    column = (global_ids % total_lon - sector_here * blocks_here + 1) % total_lon
    near_step = jnp.where(band_here % 2 == 0, 1, -1)
    group = jnp.where(band_step == 0, 0, jnp.where(band_step == near_step, 1, 2))
    even = sector_here % 2 == 0
    outer_column = jnp.where(even, 0, blocks_here + 1)
    inner_column = jnp.where(even, blocks_here, 1)
    at_outer = column == jnp.where(even, 1, blocks_here)
    outer_first = jnp.where(at_outer, 0, jnp.where(column == inner_column, 1, column))
    if own_in_order:
        outer_first = jnp.where(group == 0, column - 1, outer_first)
    inside = group * blocks_here + outer_first
    is_outer = column == outer_column
    outside = 3 * blocks_here + jnp.where(
        group == 2, jnp.where(is_outer, 4, 5), jnp.where(is_outer, 0, 2) + group
    )
    own_column = jnp.logical_and(column >= 1, column <= blocks_here)
    return jnp.where(own_column, inside, outside)


def fill_table(pieces, table, sems):
    copies = []
    start = 0
    for place, piece in enumerate(pieces):
        count = piece.shape[0]
        copies.append(pltpu.make_async_copy(piece, table.at[pl.ds(start, count)], sems.at[place]))
        start += count
    return copies


def normalise(values, gain):
    centred = values - jnp.mean(values, axis=-1, keepdims=True)
    spread = jnp.mean(centred * centred, axis=-1, keepdims=True)
    return (centred * lax.rsqrt(spread + EPSILON) * gain).astype(jnp.bfloat16)


def two_parts(values):
    upper = lax.reduce_precision(values, 8, 7)
    return upper.astype(jnp.bfloat16), (values - upper).astype(jnp.bfloat16)


def stacked_weights(weight):
    count, picks, rows, width = weight.shape
    wide = weight.transpose(0, 2, 1, 3).reshape(count, rows, picks * width)
    return jnp.concatenate(two_parts(wide), axis=1)


def mix_blocks(slots, place, split, table, upper, lower):
    width = table.shape[1]
    rows = split.shape[0] // 2
    for k in range(split.shape[1] // width):
        block = table[slots[place, k]]
        high = block.astype(jnp.bfloat16)
        upper[k * width:(k + 1) * width, :] = high
        if lower is not None:
            lower[k * width:(k + 1) * width, :] = (block - high.astype(jnp.float32)).astype(jnp.bfloat16)
    both = jnp.dot(split[...], upper[...], preferred_element_type=jnp.float32)
    total = both[:rows] + both[rows:]
    if lower is not None:
        total = total + jnp.dot(split[0:rows, :], lower[...], preferred_element_type=jnp.float32)
    return total


def block_at(place, count, even):
    first = jnp.where(even[0] == 1, 0, count - 1)
    return jnp.where(place == 0, first, jnp.where(place == 1, count - 1 - first, place - 1))


def lift_kernel(slots, even, *refs, piece_count):
    pieces = refs[:piece_count]
    split, gains, mesh_in, *rest = refs[piece_count:]
    table, upper, lower, sems = rest[-4:]
    parts = rest[:-4]
    copies = fill_table(pieces, table, sems)
    for copy in copies:
        copy.start()
    for copy in copies:
        copy.wait()
    for m, part in enumerate(parts):
        source = block_at(m, len(parts), even)
        mixed = mix_blocks(slots, source, split.at[source], table, upper, lower)
        mesh_in[m] = mixed
        part[0] = normalise(mixed, gains[0:1, :])


def return_kernel(slots, *refs, piece_count):
    pieces = refs[:piece_count]
    split, out, table, upper, sems = refs[piece_count:]
    copies = fill_table(pieces, table, sems)
    for copy in copies:
        copy.start()
    for copy in copies:
        copy.wait()
    for g in range(split.shape[0]):
        out[g] = mix_blocks(slots, g, split.at[g], table, upper, None)


def layer_kernel(slots, counts, even, *refs, piece_count):
    pieces = refs[:piece_count]
    queries, mesh_in, gains, out_hbm, up_hbm, down_hbm, *rest = refs[piece_count:]
    table, keys, values, mixed, out_weight, up_weight, down_weight, sems = rest[-8:]
    parts = rest[:-8]
    copies = fill_table(pieces, table, sems)
    weights = [
        pltpu.make_async_copy(out_hbm, out_weight, sems.at[piece_count]),
        pltpu.make_async_copy(up_hbm, up_weight, sems.at[piece_count + 1]),
        pltpu.make_async_copy(down_hbm, down_weight, sems.at[piece_count + 2]),
    ]
    for copy in copies + weights:
        copy.start()
    for copy in copies:
        copy.wait()
    mesh_blocks, rows, width = mesh_in.shape
    neighbours = keys.shape[0] // rows
    head_size = width // HEADS
    wide = 2 * head_size
    low_half = lax.broadcasted_iota(jnp.int32, (rows, wide), 1) < head_size
    key_block = lax.broadcasted_iota(jnp.int32, (neighbours * rows, wide), 0) // rows
    first_lane = lax.broadcasted_iota(jnp.int32, (2 * rows, wide), 1) == 0
    marker = jnp.where(first_lane, 1.0, 0.0).astype(jnp.bfloat16)
    values[:, :, wide:] = jnp.ones((HEADS // 2, neighbours * rows, wide), jnp.bfloat16)

    def attend(m, carry):
        source = block_at(m, mesh_blocks, even)
        for j in range(neighbours):
            slot = slots[source, j]
            keys[j * rows:(j + 1) * rows, :] = table[slot, :, 0:width]
            for h in range(HEADS // 2):
                at = width + h * wide
                values[h, j * rows:(j + 1) * rows, 0:wide] = table[slot, :, at:at + wide]
        bias = jnp.where(key_block < counts[source], 0.0, -1e30).astype(jnp.bfloat16)

        def score(h):
            at = h * wide
            query = queries[m, :, at:at + wide] * jnp.asarray(head_size ** (-0.5), jnp.bfloat16)
            none = jnp.zeros_like(query)
            pair_rows = jnp.concatenate(
                [jnp.where(low_half, query, none), jnp.where(low_half, none, query)], axis=0
            )
            return lax.dot_general(
                jnp.concatenate([pair_rows, marker], axis=1),
                jnp.concatenate([keys[:, at:at + wide], bias], axis=1),
                (((1,), (1,)), ((), ())),
                preferred_element_type=jnp.float32,
            )

        following = score(0)
        for h in range(HEADS // 2):
            at = h * wide
            scores = following
            if h + 1 < HEADS // 2:
                following = score(h + 1)
            highest = jnp.max(scores, axis=-1, keepdims=True)
            raw = jnp.exp(scores - highest).astype(jnp.bfloat16)
            summed = jnp.dot(raw, values[h], preferred_element_type=jnp.float32)
            part = summed[:, :wide] / summed[:, wide:]
            mixed[pl.ds(m * rows, rows), at:at + wide] = jnp.where(
                low_half, part[:rows], part[rows:]
            ).astype(jnp.bfloat16)
        return carry

    lax.fori_loop(0, mesh_blocks, attend, 0)
    for copy in weights:
        copy.wait()
    after = mesh_in[...].reshape(mesh_blocks * rows, width) + jnp.dot(
        mixed[...], out_weight[...], preferred_element_type=jnp.float32
    )
    again = normalise(after, gains[1:2, :])
    hidden = jnp.dot(again, up_weight[...], preferred_element_type=jnp.float32)
    hidden = (0.5 * hidden * (1.0 + lax.erf(hidden * 0.7071067811865476))).astype(jnp.bfloat16)
    result = after + jnp.dot(hidden, down_weight[...], preferred_element_type=jnp.float32)
    result = result.astype(jnp.bfloat16).reshape(mesh_blocks, rows, width)
    for m in range(mesh_blocks):
        parts[m][0] = result[m]


def any_specs(count):
    return [pl.BlockSpec(memory_space=pl.ANY)] * count


VMEM_SPEC = pl.BlockSpec(memory_space=pltpu.MemorySpace.VMEM)


def shards(
    grid_feats, lift_index, lift_weight, window_index, window_count, norm_gains,
    qkv_weight, out_weight, up_weight, down_weight, return_index, return_weight,
):
    even_sector = lax.axis_index("lon") % 2 == 0
    lon_count = lax.axis_size("lon")
    grid_blocks = grid_feats.shape[1]
    mesh_blocks = lift_index.shape[1]
    rows, width = grid_feats.shape[2:]
    grid_lon = grid_blocks * lon_count
    mesh_lon = mesh_blocks * lon_count
    bf16, f32 = jnp.bfloat16, jnp.float32
    mesh_table = 3 * mesh_blocks + 6
    grid_table = 3 * grid_blocks + 6

    even = even_sector.astype(jnp.int32).reshape(1)
    part_shapes = [jax.ShapeDtypeStruct((1, rows, width), bf16)] * mesh_blocks
    own_grid = grid_feats[0]
    sent = []
    for i in range(grid_blocks):
        mirror = grid_blocks - 1 - i
        chosen = jnp.where(even_sector, own_grid[i:i + 1], own_grid[mirror:mirror + 1])
        sent.append((chosen * GRID_SCALE).astype(jnp.float16))
    near, far, side, last = exchange(sent)

    def decode(pieces):
        return [piece.astype(f32) * (1.0 / GRID_SCALE) for piece in pieces]

    grid_pieces = [own_grid] + decode(near) + decode(far)
    grid_pieces += decode(side) + decode(last)
    lift_slots = table_slots(lift_index[0], grid_lon, grid_blocks, True)
    picks = lift_weight.shape[2]
    mesh_in, *parts = pl.pallas_call(
        lambda *refs: lift_kernel(*refs, piece_count=len(grid_pieces)),
        grid_spec=pltpu.PrefetchScalarGridSpec(
            num_scalar_prefetch=2,
            in_specs=any_specs(len(grid_pieces)) + [VMEM_SPEC, VMEM_SPEC],
            out_specs=[VMEM_SPEC] * (1 + mesh_blocks),
            scratch_shapes=[
                pltpu.VMEM((grid_table, rows, width), f32),
                pltpu.VMEM((picks * rows, width), bf16),
                pltpu.VMEM((picks * rows, width), bf16),
                pltpu.SemaphoreType.DMA((len(grid_pieces),)),
            ],
        ),
        out_shape=[
            jax.ShapeDtypeStruct((mesh_blocks, rows, width), f32),
        ] + part_shapes,
        compiler_params=pltpu.CompilerParams(vmem_limit_bytes=20 * MEBI),
        name="lift",
    )(lift_slots, even, *grid_pieces, stacked_weights(lift_weight[0]), norm_gains)

    near, far, side, last = exchange(parts)
    normed = jnp.concatenate(parts, axis=0)
    own = jnp.dot(normed.reshape(-1, width), qkv_weight, preferred_element_type=f32).astype(bf16)
    queries = own[:, :width].reshape(mesh_blocks, rows, width)
    kv_weight = qkv_weight[:, width:]
    kv_pieces = [own[:, width:].reshape(mesh_blocks, rows, 2 * width)]

    def project(group):
        stacked = jnp.concatenate(group, axis=0) if len(group) > 1 else group[0]
        return (
            jnp.dot(stacked.reshape(-1, width), kv_weight, preferred_element_type=f32)
            .astype(bf16)
            .reshape(-1, rows, 2 * width)
        )

    kv_pieces.append(project(near))
    side = project(side)
    kv_pieces.append(project(far))
    kv_pieces += [side, project(last)]
    window_slots = table_slots(window_index[0], mesh_lon, mesh_blocks, False)
    neighbours = window_index.shape[2]
    hidden_width = up_weight.shape[1]
    parts = pl.pallas_call(
        lambda *refs: layer_kernel(*refs, piece_count=len(kv_pieces)),
        grid_spec=pltpu.PrefetchScalarGridSpec(
            num_scalar_prefetch=3,
            in_specs=any_specs(len(kv_pieces)) + [VMEM_SPEC] * 3 + any_specs(3),
            out_specs=[VMEM_SPEC] * mesh_blocks,
            scratch_shapes=[
                pltpu.VMEM((mesh_table, rows, 2 * width), bf16),
                pltpu.VMEM((neighbours * rows, width), bf16),
                pltpu.VMEM((HEADS // 2, neighbours * rows, 4 * (width // HEADS)), bf16),
                pltpu.VMEM((mesh_blocks * rows, width), bf16),
                pltpu.VMEM((width, width), bf16),
                pltpu.VMEM((width, hidden_width), bf16),
                pltpu.VMEM((hidden_width, width), bf16),
                pltpu.SemaphoreType.DMA((len(kv_pieces) + 3,)),
            ],
        ),
        out_shape=part_shapes,
        compiler_params=pltpu.CompilerParams(vmem_limit_bytes=42 * MEBI),
        name="layer",
    )(
        window_slots, window_count[0], even, *kv_pieces, queries, mesh_in, norm_gains,
        out_weight, up_weight, down_weight,
    )

    near, far, side, last = exchange(parts)
    mesh_pieces = list(parts) + near + far + side + last
    return_slots = table_slots(return_index[0], mesh_lon, mesh_blocks, False)
    grid_out = pl.pallas_call(
        lambda *refs: return_kernel(*refs, piece_count=len(mesh_pieces)),
        grid_spec=pltpu.PrefetchScalarGridSpec(
            num_scalar_prefetch=1,
            in_specs=any_specs(len(mesh_pieces)) + [VMEM_SPEC],
            out_specs=VMEM_SPEC,
            scratch_shapes=[
                pltpu.VMEM((mesh_table, rows, width), bf16),
                pltpu.VMEM((picks * rows, width), bf16),
                pltpu.SemaphoreType.DMA((len(mesh_pieces),)),
            ],
        ),
        out_shape=jax.ShapeDtypeStruct((grid_blocks, rows, width), f32),
        compiler_params=pltpu.CompilerParams(vmem_limit_bytes=16 * MEBI),
        name="give_back",
    )(return_slots, *mesh_pieces, stacked_weights(return_weight[0]))
    return grid_out.reshape(1, grid_blocks, rows, width)


def solution(mesh):
    placed = (
        P("lat", "lon", None, None),
        P("lat", "lon", None),
        P("lat", "lon", None, None, None),
        P("lat", "lon", None),
        P("lat", "lon"),
        P(),
        P(),
        P(),
        P(),
        P(),
        P("lat", "lon", None),
        P("lat", "lon", None, None, None),
    )

    return jax.shard_map(
        shards, mesh=mesh, in_specs=placed, out_specs=P("lat", "lon", None, None), check_vma=False
    )
```
